256 devices in a mesh: lon: 32 (over x, y, core), lat: 8 (over z).
Axes of the slice: x: 4, y: 4, z: 8, core: 2. Of those that a mesh axis runs over, the one named last changes fastest.
Arguments:
- surface_forcing: float32 [192, 4096], P('lat', 'lon'), may hold values from -33 to 33
- sea_mask: int32 [192, 4096], P('lat', 'lon'), may hold values 0 or 1
- level_count: int32 [192, 4096], P('lat', 'lon'), may hold values from 1 to 40
- state: float32 [4, 40, 192, 4096], P(None, None, 'lat', 'lon'), may hold values from -6 to 6
Outputs:
- surface_height: float32 [192, 4096], P('lat', 'lon')
- residual: float32 [192, 4096], P('lat', 'lon')
- tendency: float32 [4, 40, 192, 4096], P(None, None, 'lat', 'lon')
The draws below stay inside these ranges and needn't reach their ends.
All inputs are finite; a program needn't handle non-finite values. No bound on the sum of `sea_mask` on one device may be relied on, other than what follows from the above.
Results may differ from the reference program's by a relative error of at most 0.0003.
Values sent between devices are 32-bit elements; how exact they have to be, the bound alone decides.
A program may use at most 64 MiB of HBM per device.

```python
import jax
import jax.numpy as jnp
from jax import lax

LEV = 40
ITERS = 4
NX = 4096
NY = 192


def draw_surface_forcing(key, part):
    row_frac = jnp.arange(NY, dtype=jnp.float32) / NY
    column_frac = jnp.arange(NX, dtype=jnp.float32) / NX
    growth = jnp.exp(jnp.log(3.0) * (row_frac[:, None] + column_frac[None, :]))
    key_rough = jax.random.fold_in(jax.random.fold_in(key, 11), 0)
    values = jax.random.truncated_normal(key_rough, -3.0, 3.0, (NY, NX), jnp.float32) * growth
    return values


def plant(values, own_key, least, top_value):
    spot = [jax.random.randint(jax.random.fold_in(own_key, axis), (), 0, length) for axis, length in enumerate(values.shape)]
    main_axis = values.shape.index(max(values.shape))
    neighbour = spot[:main_axis] + [(spot[main_axis] + 1) % values.shape[main_axis]] + spot[main_axis + 1:]
    return values.at[tuple(spot)].set(least).at[tuple(neighbour)].set(top_value)


def shard_levels(key, shape, pieces, low, largest):
    def one(axis_at, parts):
        draws = jax.random.uniform(jax.random.fold_in(jax.random.fold_in(key, 6), axis_at), (parts,), jnp.float32, low / len(pieces), largest / len(pieces))
        return jnp.repeat(jnp.exp(draws), shape[axis_at] // parts).reshape((-1,) + (1,) * (len(shape) - axis_at - 1))

    gain = one(*pieces[0])
    for cut in pieces[1:]:
        gain = gain * one(*cut)
    return gain


def centred(key, dims, scale, most, cuts=(), kind=jnp.bfloat16):
    entries = scale * jax.random.normal(key, dims, jnp.float32)
    if cuts:
        entries = entries * shard_levels(key, dims, cuts, -0.22, 0.18)
    return jnp.clip(entries, -most, most).astype(kind)


def setup_inputs(seed: int = 0) -> dict:
    arg_keys = jax.random.split(jax.random.key(seed), 5)
    return {
        "surface_forcing": draw_surface_forcing(jax.random.fold_in(arg_keys[4], 71), 0),
        "sea_mask": plant((jax.random.randint(arg_keys[1], (NY, NX), 0, 4) < 3).astype(jnp.int32), jax.random.fold_in(arg_keys[1], 1), 0, 1),
        "level_count": plant(jax.random.randint(arg_keys[2], (NY, NX), 1, LEV + 1), jax.random.fold_in(arg_keys[2], 1), 1, LEV).astype(jnp.int32),
        "state": centred(arg_keys[3], (4, LEV, NY, NX), 1.0, 6.0, ((2, 8), (3, 32)), jnp.float32),
    }


damping = 0.05
face_scale = 1.0
viscosity = 0.02


def wrap_pad(field, width):
    field = jnp.concatenate([field[..., -width:], field, field[..., :width]], axis=-1)
    spec = [(0, 0)] * (field.ndim - 2) + [(width, width), (0, 0)]
    return jnp.pad(field, spec)


def trim_rims(field, margin):
    return field[..., margin:field.shape[-2] - margin, margin:field.shape[-1] - margin]


def face_coeffs(depth, width_out, width_in):
    offset = width_in - width_out
    height = depth.shape[0] - 2 * offset
    breadth = depth.shape[1] - 2 * offset
    center = depth[offset:offset + height, offset:offset + breadth]
    east_face = face_scale * jnp.minimum(center, depth[offset:offset + height, offset + 1:offset + 1 + breadth])
    west_face = face_scale * jnp.minimum(center, depth[offset:offset + height, offset - 1:offset - 1 + breadth])
    north_face = face_scale * jnp.minimum(center, depth[offset + 1:offset + 1 + height, offset:offset + breadth])
    south_face = face_scale * jnp.minimum(center, depth[offset - 1:offset - 1 + height, offset:offset + breadth])
    diagonal = damping + east_face + west_face + north_face + south_face
    return diagonal, east_face, west_face, north_face, south_face


def operator_apply(padded, coeffs):
    diagonal, east_face, west_face, north_face, south_face = coeffs
    return (diagonal * padded[1:-1, 1:-1] - east_face * padded[1:-1, 2:] - west_face * padded[1:-1, :-2]
            - north_face * padded[2:, 1:-1] - south_face * padded[:-2, 1:-1])


def laplace(field, active):
    center = field[..., 1:-1, 1:-1]
    active_center = active[..., 1:-1, 1:-1]
    east_part = active_center * active[..., 1:-1, 2:] * (field[..., 1:-1, 2:] - center)
    west_part = active_center * active[..., 1:-1, :-2] * (center - field[..., 1:-1, :-2])
    north_part = active_center * active[..., 2:, 1:-1] * (field[..., 2:, 1:-1] - center)
    south_part = active_center * active[..., :-2, 1:-1] * (center - field[..., :-2, 1:-1])
    return east_part - west_part + north_part - south_part


def advect(field, active):
    east_flow = field[2]
    north_flow = field[3]
    center = field[..., 1:-1, 1:-1]
    active_center = active[..., 1:-1, 1:-1]
    flow_center = east_flow[..., 1:-1, 1:-1]
    lift_center = north_flow[..., 1:-1, 1:-1]
    east_speed = 0.25 * active_center * active[..., 1:-1, 2:] * (flow_center + east_flow[..., 1:-1, 2:])
    west_speed = 0.25 * active_center * active[..., 1:-1, :-2] * (flow_center + east_flow[..., 1:-1, :-2])
    north_speed = 0.25 * active_center * active[..., 2:, 1:-1] * (lift_center + north_flow[..., 2:, 1:-1])
    south_speed = 0.25 * active_center * active[..., :-2, 1:-1] * (lift_center + north_flow[..., :-2, 1:-1])
    return (east_speed * (center + field[..., 1:-1, 2:]) - west_speed * (center + field[..., 1:-1, :-2])
            + north_speed * (center + field[..., 2:, 1:-1]) - south_speed * (center + field[..., :-2, 1:-1]))


def tendency_of(state_wide, active_wide):
    inner_active = trim_rims(active_wide, 1)
    smoothed = laplace(laplace(state_wide, active_wide), inner_active)
    flux = advect(trim_rims(state_wide, 1), inner_active)
    return trim_rims(active_wide, 2) * (-flux - viscosity * smoothed)


def reference(surface_forcing, sea_mask, level_count, state):
    sea = sea_mask.astype(jnp.float32)
    depth = sea * level_count.astype(jnp.float32) / LEV
    coeffs = face_coeffs(wrap_pad(depth, 1), 0, 1)
    forcing = sea * surface_forcing
    solution = jnp.zeros_like(forcing)
    residual = forcing
    search = residual / coeffs[0]
    direction = search
    product = jnp.sum(residual * search)
    for step_index in range(ITERS):
        image = operator_apply(wrap_pad(direction, 1), coeffs)
        alpha_step = product / jnp.sum(direction * image)
        solution = solution + alpha_step * direction
        residual = residual - alpha_step * image
        if step_index + 1 < ITERS:
            search = residual / coeffs[0]
            product_next = jnp.sum(residual * search)
            direction = search + (product_next / product) * direction
            product = product_next

    def level_tendency(level):
        active = (level < level_count).astype(jnp.float32) * sea
        layer = lax.dynamic_index_in_dim(state, level, 1, keepdims=False)
        return tendency_of(wrap_pad(layer, 2), wrap_pad(active, 2))

    stacked = lax.map(level_tendency, jnp.arange(LEV, dtype=jnp.int32))
    return solution, residual, jnp.moveaxis(stacked, 0, 1)
```

```python
import jax
import jax.numpy as jnp
from jax import lax
from jax.experimental import pallas as pl
from jax.experimental.pallas import tpu as pltpu
from jax.sharding import PartitionSpec as P

MESH = pl.DeviceIdType.MESH
F32 = jnp.float32
CORES = 2
GROUP = 16
VISC = 0.02
DIRS = ((1, 0), (-1, 0), (0, 1), (0, -1), (1, 1), (-1, -1), (1, -1), (-1, 1))
OPP = (1, 0, 3, 2, 5, 4, 7, 6)
E, W, N, S, NE, SW, SE, NW = range(8)


def two_sum(a, b):
    s = a + b
    t = s - a
    return s, (a - (s - t)) + (b - t)


def quick(a, b):
    s = a + b
    return s, b - (s - a)


def split(a):
    t = 4097.0 * a
    h = t - (t - a)
    return h, a - h


def two_prod(a, b):
    p = a * b
    ah, al = split(a)
    bh, bl = split(b)
    return p, ((ah * bh - p) + ah * bl + al * bh) + al * bl


def int_prod(w, h):
    p = w * h
    a, b = split(h)
    return p, (w * a - p) + w * b


def dd_add(a, b):
    s, e = two_sum(a[0], b[0])
    return quick(s, e + (a[1] + b[1]))


def dd_mul(a, b):
    p, e = two_prod(a[0], b[0])
    return quick(p, e + (a[0] * b[1] + a[1] * b[0]))


def dd_neg(a):
    return -a[0], -a[1]


def dd_div(a, b):
    r = 1.0 / b[0]
    q = a[0] * r
    p, e = two_prod(q, b[0])
    rest = ((a[0] - p) - e) + (a[1] - q * b[1])
    return quick(q, rest * r)


def iota(shape, dim):
    return lax.broadcasted_iota(jnp.int32, shape, dim)


def shift_rows(x, step):
    return pltpu.roll(x, (-step) % x.shape[0], 0)


def shift_lanes(x, step):
    return pltpu.roll(x, (-step) % 128, 1)


def cg_coefficients(mu):
    s, t = dict(enumerate(mu)), dict(enumerate(mu))
    one = (jnp.ones_like(mu[0][0]), jnp.zeros_like(mu[0][0]))
    p, q = [one], [one]
    x = []
    for k in range(4):
        alpha = dd_div(s[k], t[k + 1])
        minus = dd_neg(alpha)
        x = [dd_add(x[i], dd_mul(alpha, q[i])) if i < len(x) else dd_mul(alpha, q[i]) for i in range(k + 1)]
        moved = [dd_mul(minus, c) for c in q]
        p = [p[i] if i == 0 else (dd_add(p[i], moved[i - 1]) if i <= k else moved[i - 1]) for i in range(k + 2)]
        if k < 3:
            last = 6 - k
            s_next = {j: dd_add(s[j], dd_mul(minus, t[j + 1])) for j in range(k + 1, last + 1)}
            beta = dd_mul(minus, dd_div(s_next[k + 1], s[k]))
            t = {j: dd_add(s_next[j], dd_mul(beta, t[j])) for j in range(k + 2, last + 1)}
            s = s_next
            q = [dd_add(p[i], dd_mul(beta, q[i])) if i <= k else p[i] for i in range(k + 2)]
    return x, p


def tendencies(active, quads):
    east = shift_lanes(active, 1)
    north = shift_rows(active, 1)
    face_e = active * east
    face_n = active * north
    count = face_e + shift_lanes(face_e, -1) + face_n + shift_rows(face_n, -1)
    u, v = quads[2], quads[3]
    flow_e = (0.25 * face_e) * (u + shift_lanes(u, 1))
    flow_n = (0.25 * face_n) * (v + shift_rows(v, 1))
    own = slice(0, 24)
    flow_w = shift_lanes(flow_e, -1)[own]
    flow_s = shift_rows(flow_n, -1)[own]
    flow_e, flow_n = flow_e[own], flow_n[own]
    net = (flow_e - flow_w) + (flow_n - flow_s)
    out = []
    for q in quads:
        q = active * q
        qe, qw, qn, qs = shift_lanes(q, 1), shift_lanes(q, -1), shift_rows(q, 1), shift_rows(q, -1)
        lap = active * ((qe + qw) + (qn + qs)) - count * q
        around = (shift_lanes(lap, 1) + shift_lanes(lap, -1)) + (shift_rows(lap, 1) + shift_rows(lap, -1))
        flux = (net * q[own] + flow_e * qe[own]) + (flow_n * qn[own] - flow_w * qw[own]) - flow_s * qs[own]
        out.append(VISC * (count[own] * lap[own] - active[own] * around[own]) - flux)
    return out


def make_kernel(nlon, nlat, levels, names):
    nplane = nlon // CORES
    nline = CORES * nlat
    groups = -(-levels // GROUP)
    entries = levels + groups
    order = [names.index("lon"), names.index("lat")]

    def device(lon, lat):
        pair = (lon, lat)
        return (pair[order.index(0)], pair[order.index(1)])

    def kernel(forcing_hbm, sea_hbm, count_hbm, state_hbm, x_ref, r_ref, tend_hbm,
               forcing, sea, count, state, tend, surf, surf_ew, surf_ns, edges, edges_in, rows_up, rows_down,
               rows_in, corners_in, edge_out, partial, gather_a, mid, gather_b,
               in_sem, out_sem, send_sem, recv_sem, send_a, recv_a, send_b, recv_b):
        lon = lax.axis_index("lon")
        lat = lax.axis_index("lat")
        plane, core = lon // CORES, lon % CORES
        line = core * nlat + lat

        small = [pltpu.make_async_copy(a, b, in_sem.at[i]) for i, (a, b) in
                 enumerate(((forcing_hbm, forcing), (sea_hbm, sea), (count_hbm, count)))]
        large = [pltpu.make_async_copy(state_hbm.at[f], state.at[f], in_sem.at[3 + f]) for f in range(4)]
        for copy in small + large:
            copy.start()

        near = [device((lon + dx + nlon) % nlon, (lat + dy + nlat) % nlat) for dx, dy in DIRS]
        plane_peer = [device(((plane + j) % nplane) * CORES + core, lat) for j in range(1, nplane)]
        line_peer = []
        for j in range(1, nline):
            other = (line + j) % nline
            line_peer.append(device(plane * CORES + other // nlat, other % nlat))
        barrier = pltpu.get_barrier_semaphore()
        peers = near + plane_peer + line_peer
        for peer in peers:
            pl.semaphore_signal(barrier, inc=1, device_id=peer, device_id_type=MESH)

        lane = iota((8, 128), 1)
        sub = iota((8, 128), 0)

        for copy in small:
            copy.wait()
        wet = sea[...] * count[...]
        for t in range(3):
            rows = slice(8 * t, 8 * t + 8)
            surf[t, 0] = wet[rows].astype(F32)
            surf[t, 1] = (sea[rows].astype(F32) * forcing[rows]) * 65536.0

        for copy in large:
            copy.wait()

        lane24 = iota((24, 128), 1)

        def pack_edges(f, carry):
            for g in range(groups):
                packed = jnp.zeros((24, 128), F32)
                for i in range(min(GROUP, levels - g * GROUP)):
                    moved = pltpu.roll(state[f, g * GROUP + i], (4 + 8 * i) % 128, 1)
                    packed = jnp.where(lane24 // 8 == i, moved, packed)
                edges[f, g] = packed
            return carry

        lax.fori_loop(0, 4, pack_edges, 0)

        def packed_rows(tile_of):
            up, down = None, None
            for f in range(4):
                top = pltpu.roll(tile_of(f, slice(16, 24)), (2 * f + 2) % 8, 0)
                low = tile_of(f, slice(0, 8))
                low = pltpu.roll(low, 2 * f, 0) if f else low
                up = top if f == 0 else jnp.where(sub // 2 == f, top, up)
                down = low if f == 0 else jnp.where(sub // 2 == f, low, down)
            return up, down

        def pack_rows(k, carry):
            up, down = packed_rows(lambda f, rows: state[f, k, rows])
            rows_up[k] = up
            rows_down[k] = down
            return carry

        lax.fori_loop(0, levels, pack_rows, 0)
        for g in range(groups):
            up, down = packed_rows(lambda f, rows: edges[f, g, rows])
            rows_up[levels + g] = up
            rows_down[levels + g] = down

        pl.semaphore_wait(barrier, len(peers))

        def surf_slot(d):
            return surf_ew.at[d] if d < 2 else surf_ns.at[d - 2]

        def surf_copy(d):
            source = surf if d < 2 else surf.at[2 if DIRS[d][1] > 0 else 0]
            return pltpu.make_async_remote_copy(source, surf_slot(OPP[d]), send_sem.at[d], recv_sem.at[OPP[d]],
                                                device_id=near[d], device_id_type=MESH)

        def rows_copy(d):
            source = rows_up if DIRS[d][1] > 0 else rows_down
            if d < 4:
                target = rows_in.at[OPP[d] - 2]
            else:
                source, target = source.at[pl.ds(levels, groups)], corners_in.at[OPP[d] - 4]
            return pltpu.make_async_remote_copy(source, target, send_sem.at[8 + d], recv_sem.at[8 + OPP[d]],
                                                device_id=near[d], device_id_type=MESH)

        def edge_copy(d):
            return pltpu.make_async_remote_copy(edges, edges_in.at[OPP[d]], send_sem.at[8 + d], recv_sem.at[8 + OPP[d]],
                                                device_id=near[d], device_id_type=MESH)

        surf_copies = [surf_copy(d) for d in range(8)]
        other_copies = [edge_copy(d) if d < 2 else rows_copy(d) for d in range(8)]
        for copy in surf_copies + other_copies:
            copy.start()
        for copy in surf_copies:
            copy.wait_recv()

        has_north = jnp.where(lat < nlat - 1, 1.0, 0.0).astype(F32)
        has_south = jnp.where(lat > 0, 1.0, 0.0).astype(F32)

        def wide(v):
            own = [surf[t, v] for t in range(3)] + [surf_ns[N - 2, v] * has_north, surf_ns[S - 2, v] * has_south]
            side = [jnp.where(lane < 64, surf_ew[E, t, v], surf_ew[W, t, v]) for t in range(3)]
            side.append(jnp.where(lane < 64, surf_ns[NE - 2, v], surf_ns[NW - 2, v]) * has_north)
            side.append(jnp.where(lane < 64, surf_ns[SE - 2, v], surf_ns[SW - 2, v]) * has_south)
            return jnp.concatenate(own, 0), jnp.concatenate(side, 0)

        lane40 = iota((40, 128), 1)

        def to_east(pair):
            a, b = shift_lanes(pair[0], 1), shift_lanes(pair[1], 1)
            return jnp.where(lane40 == 127, b, a), jnp.where(lane40 == 127, a, b)

        def to_west(pair):
            a, b = shift_lanes(pair[0], -1), shift_lanes(pair[1], -1)
            return jnp.where(lane40 == 0, b, a), jnp.where(lane40 == 0, a, b)

        def to_north(pair):
            return shift_rows(pair[0], 1), shift_rows(pair[1], 1)

        def to_south(pair):
            return shift_rows(pair[0], -1), shift_rows(pair[1], -1)

        moves = (to_east, to_west, to_north, to_south)
        depth = wide(0)
        force = wide(1)
        moved = [move(depth) for move in moves]
        faces = [[jnp.minimum(depth[t], m[t]) for m in moved] for t in range(2)]
        diag = [2.0 + ((faces[t][0] + faces[t][1]) + (faces[t][2] + faces[t][3])) for t in range(2)]
        inverse = [1.0 / diag[t] for t in range(2)]

        def over_diag(hi, lo, t):
            q = hi * inverse[t]
            a, b = split(q)
            rest = ((hi - diag[t] * a) - diag[t] * b) + lo
            return q, rest * inverse[t]

        vectors = [[quick(*over_diag(force[t], jnp.zeros_like(force[t]), t)) for t in range(2)]]
        for k in range(4):
            last = vectors[-1]
            high = [move((last[0][0], last[1][0])) for move in moves]
            low = [move((last[0][1], last[1][1])) for move in moves]
            following = []
            for t in range(2):
                if k == 3 and t == 1:
                    continue
                terms = [int_prod(faces[t][i], high[i][t]) for i in range(4)]
                fine = [faces[t][i] * low[i][t] + terms[i][1] for i in range(4)]
                s0, e0 = two_sum(terms[0][0], terms[1][0])
                s1, e1 = two_sum(terms[2][0], terms[3][0])
                s, e2 = two_sum(s0, s1)
                rest = ((e0 + e1) + e2) + ((fine[0] + fine[1]) + (fine[2] + fine[3]))
                q, q_low = over_diag(s, rest, t)
                s, e = two_sum(last[t][0], -q)
                following.append(quick(s, e + (last[t][1] - q_low)))
            vectors.append(following)
        own_vectors = [(v[0][0][:24], v[0][1][:24]) for v in vectors]
        own_diag = diag[0][:24]

        sums = []
        for n in range(8):
            a, b = own_vectors[n // 2], own_vectors[n - n // 2]
            p, e = int_prod(own_diag, a[0])
            product = dd_mul(quick(p, e + own_diag * a[1]), b)
            tiles = [(product[0][8 * i:8 * i + 8], product[1][8 * i:8 * i + 8]) for i in range(3)]
            sums.append(dd_add(dd_add(tiles[0], tiles[1]), tiles[2]))

        def fold(a, b, near_mask, step):
            def one(i):
                x, y = a[i], b[i]
                far = jnp.where(near_mask, pltpu.roll(x, 8 - step, 0), pltpu.roll(y, step, 0))
                return jnp.where(near_mask, x, y), far
            kept, far = zip(*(one(i) for i in range(2)))
            return dd_add(kept, far)

        level = [fold(sums[2 * i], sums[2 * i + 1], sub < 4, 4) for i in range(4)]
        level = [fold(level[2 * i], level[2 * i + 1], sub % 4 < 2, 2) for i in range(2)]
        level = fold(level[0], level[1], sub % 2 < 1, 1)
        far = (pltpu.roll(level[0], 64, 1), pltpu.roll(level[1], 64, 1))
        level = dd_add(level, far)
        partial[...] = jnp.where(lane < 64, level[0], level[1])

        copies_a = [pltpu.make_async_remote_copy(partial, gather_a.at[j], send_a.at[j], recv_a.at[j],
                                                 device_id=plane_peer[j], device_id_type=MESH)
                    for j in range(nplane - 1)]
        for copy in copies_a:
            copy.start()

        def unpacked(message):
            return message, pltpu.roll(message, 64, 1)

        def total(messages):
            parts = [unpacked(m) for m in messages]
            while len(parts) > 1:
                parts = [dd_add(parts[i], parts[i + 1]) if i + 1 < len(parts) else parts[i]
                         for i in range(0, len(parts), 2)]
            return parts[0]

        for d in (N, S):
            other_copies[d].wait_recv()
        count_own = jnp.concatenate([depth[0][:24], jnp.where(sub < 4, depth[0][24:32], depth[0][32:40])], 0)
        count_side = jnp.concatenate([depth[1][:24], jnp.where(sub < 4, depth[1][24:32], depth[1][32:40])], 0)

        def with_rows(f, block, north, south):
            up = pltpu.roll(north, (8 - 2 * f) % 8, 0) if f else north
            down = pltpu.roll(south, 6 - 2 * f, 0) if f < 3 else south
            return jnp.concatenate([block, jnp.where(sub < 4, up, down)], 0)

        def main(k, carry):
            active = jnp.where(count_own > k.astype(F32), 1.0, 0.0)
            north, south = rows_in[N - 2, k], rows_in[S - 2, k]
            quads = [with_rows(f, state[f, k], north, south) for f in range(4)]
            for f, value in enumerate(tendencies(active, quads)):
                tend[f, k] = value
            return carry

        lax.fori_loop(0, levels, main, 0)

        for copy in copies_a:
            copy.wait_recv()
        hi, lo = total([partial[...]] + [gather_a[j] for j in range(nplane - 1)])
        mid[...] = jnp.where(lane < 64, hi, pltpu.roll(lo, 64, 1))
        copies_b = [pltpu.make_async_remote_copy(mid, gather_b.at[j], send_b.at[j], recv_b.at[j],
                                                 device_id=line_peer[j], device_id_type=MESH)
                    for j in range(nline - 1)]
        for copy in copies_b:
            copy.start()

        for d in (E, W, NE, SW, SE, NW):
            other_copies[d].wait_recv()
        lane32 = iota((32, 128), 1)
        left32, left24, left8 = lane32 % 8 < 4, lane24 % 8 < 4, lane % 8 < 4

        def spread(first, second):
            x = jnp.where(lane32 < 8, jnp.where(lane32 < 4, pltpu.roll(first, 4, 1), pltpu.roll(second, 4, 1)), 0.0)
            for step in (8, 16, 32, 64):
                x = x + pltpu.roll(x, step, 1)
            return x

        count_w = spread(count_side, count_own)
        count_e = spread(count_own, count_side)

        for g in range(groups):
            kvec = (lane32 // 8 + g * GROUP).astype(F32)
            own_n, own_s = rows_in[N - 2, levels + g], rows_in[S - 2, levels + g]
            results = []
            for side in (W, E):
                if side == W:
                    counts = count_w
                    north = jnp.where(left8, corners_in[NW - 4, g], own_n)
                    south = jnp.where(left8, corners_in[SW - 4, g], own_s)
                    blocks = [jnp.where(left24, edges_in[W, f, g], edges[f, g]) for f in range(4)]
                else:
                    counts = count_e
                    north = jnp.where(left8, own_n, corners_in[NE - 4, g])
                    south = jnp.where(left8, own_s, corners_in[SE - 4, g])
                    blocks = [jnp.where(left24, edges[f, g], edges_in[E, f, g]) for f in range(4)]
                active = jnp.where(counts > kvec, 1.0, 0.0)
                results.append(tendencies(active, [with_rows(f, blocks[f], north, south) for f in range(4)]))
            for f in range(4):
                edge_out[f, g] = jnp.where(left24, results[1][f], results[0][f])

        rim = (lane24 < 2) | (lane24 >= 126)

        def blend(k, carry):
            g = k // GROUP
            back = (128 + 124 - 8 * (k % GROUP)) % 128
            for f in range(4):
                tend[f, k] = jnp.where(rim, pltpu.roll(edge_out[f, g], back, 1), tend[f, k])
            return carry

        lax.fori_loop(0, levels, blend, 0)
        out_copies = [pltpu.make_async_copy(tend.at[f], tend_hbm.at[f], out_sem.at[f]) for f in range(4)]
        for copy in out_copies:
            copy.start()

        for copy in copies_b:
            copy.wait_recv()
        level = total([mid[...]] + [gather_b[j] for j in range(nline - 1)])
        for step in (32, 16, 8, 4, 2, 1):
            level = dd_add(level, (pltpu.roll(level[0], 128 - step, 1), pltpu.roll(level[1], 128 - step, 1)))

        def scalar(a, row):
            return jnp.broadcast_to(a[row:row + 1, 0:1], (8, 128))

        mu = []
        for n in range(8):
            row = 4 * (n % 2) + 2 * (n // 2 % 2) + n // 4
            mu.append((scalar(level[0], row), scalar(level[1], row)))
        x_poly, r_poly = cg_coefficients(mu)
        for t in range(3):
            rows = slice(8 * t, 8 * t + 8)
            basis = [(v[0][rows], v[1][rows]) for v in own_vectors]

            def combined(poly):
                parts = [dd_mul(c, b) for c, b in zip(poly, basis)]
                while len(parts) > 1:
                    parts = [dd_add(parts[i], parts[i + 1]) if i + 1 < len(parts) else parts[i]
                             for i in range(0, len(parts), 2)]
                return parts[0]

            height = combined(x_poly)
            x_ref[rows] = (height[0] + height[1]) * (40.0 / 65536.0)
            rest = combined(r_poly)
            d = own_diag[rows]
            r_ref[rows] = (d * rest[0] + d * rest[1]) * (1.0 / 65536.0)

        for copy in surf_copies + other_copies + copies_a + copies_b:
            copy.wait_send()
        for copy in out_copies:
            copy.wait()

    scratch = [
        pltpu.VMEM((24, 128), F32), pltpu.VMEM((24, 128), jnp.int32), pltpu.VMEM((24, 128), jnp.int32),
        pltpu.VMEM((4, levels, 24, 128), F32), pltpu.VMEM((4, levels, 24, 128), F32),
        pltpu.VMEM((3, 2, 8, 128), F32), pltpu.VMEM((2, 3, 2, 8, 128), F32), pltpu.VMEM((6, 2, 8, 128), F32),
        pltpu.VMEM((4, groups, 24, 128), F32), pltpu.VMEM((2, 4, groups, 24, 128), F32),
        pltpu.VMEM((entries, 8, 128), F32), pltpu.VMEM((entries, 8, 128), F32),
        pltpu.VMEM((2, entries, 8, 128), F32), pltpu.VMEM((4, groups, 8, 128), F32),
        pltpu.VMEM((4, groups, 24, 128), F32),
        pltpu.VMEM((8, 128), F32), pltpu.VMEM((nplane - 1, 8, 128), F32),
        pltpu.VMEM((8, 128), F32), pltpu.VMEM((nline - 1, 8, 128), F32),
        pltpu.SemaphoreType.DMA((7,)), pltpu.SemaphoreType.DMA((4,)),
        pltpu.SemaphoreType.DMA((16,)), pltpu.SemaphoreType.DMA((16,)),
        pltpu.SemaphoreType.DMA((nplane - 1,)), pltpu.SemaphoreType.DMA((nplane - 1,)),
        pltpu.SemaphoreType.DMA((nline - 1,)), pltpu.SemaphoreType.DMA((nline - 1,)),
    ]
    return kernel, scratch


def solution(mesh):
    nlon, nlat = mesh.shape["lon"], mesh.shape["lat"]
    names = list(mesh.axis_names)

    def per_device(surface_forcing, sea_mask, level_count, state):
        kernel, scratch = make_kernel(nlon, nlat, state.shape[1], names)
        return pl.pallas_call(
            kernel,
            out_shape=(
                jax.ShapeDtypeStruct(surface_forcing.shape, F32),
                jax.ShapeDtypeStruct(surface_forcing.shape, F32),
                jax.ShapeDtypeStruct(state.shape, F32),
            ),
            in_specs=[pl.BlockSpec(memory_space=pl.ANY)] * 4,
            out_specs=(
                pl.BlockSpec(memory_space=pltpu.VMEM),
                pl.BlockSpec(memory_space=pltpu.VMEM),
                pl.BlockSpec(memory_space=pl.ANY),
            ),
            scratch_shapes=scratch,
            compiler_params=pltpu.CompilerParams(collective_id=0, has_side_effects=True),
            name="ocean",
        )(surface_forcing, sea_mask, level_count, state)

    flat, deep = P("lat", "lon"), P(None, None, "lat", "lon")
    return jax.shard_map(
        per_device, mesh=mesh, in_specs=(flat, flat, flat, deep), out_specs=(flat, flat, deep), check_vma=False
    )
```

```python
import jax
import jax.numpy as jnp
from jax import lax
from jax.experimental import pallas as pl
from jax.experimental.pallas import tpu as pltpu
from jax.sharding import Mesh
from jax.sharding import PartitionSpec as P

MESH = pl.DeviceIdType.MESH
F32 = jnp.float32
CORES = 2
GROUP = 16
VISC = 0.02
UNROLL = 2
DIRS = ((1, 0), (-1, 0), (0, 1), (0, -1), (1, 1), (-1, -1), (1, -1), (-1, 1))
OPP = (1, 0, 3, 2, 5, 4, 7, 6)
E, W, N, S, NE, SW, SE, NW = range(8)


def two_sum(a, b):
    s = a + b
    t = s - a
    return s, (a - (s - t)) + (b - t)


def quick(a, b):
    s = a + b
    return s, b - (s - a)


def split(a):
    t = 4097.0 * a
    h = t - (t - a)
    return h, a - h


def two_prod(a, b):
    p = a * b
    ah, al = split(a)
    bh, bl = split(b)
    return p, ((ah * bh - p) + ah * bl + al * bh) + al * bl


def int_prod(w, h):
    p = w * h
    a, b = split(h)
    return p, (w * a - p) + w * b


def dd_add(a, b):
    s, e = two_sum(a[0], b[0])
    return quick(s, e + (a[1] + b[1]))


def dd_mul(a, b):
    p, e = two_prod(a[0], b[0])
    return quick(p, e + (a[0] * b[1] + a[1] * b[0]))


def dd_neg(a):
    return -a[0], -a[1]


def dd_inverse(b):
    r = 1.0 / b[0]
    p, e = two_prod(r, b[0])
    rest = ((1.0 - p) - e) - r * b[1]
    return quick(r, rest * r)


def iota(shape, dim):
    return lax.broadcasted_iota(jnp.int32, shape, dim)


def shift_rows(x, step):
    return pltpu.roll(x, (-step) % x.shape[0], 0)


def shift_lanes(x, step):
    return pltpu.roll(x, (-step) % 128, 1)


def cg_coefficients(mu):
    s, t = dict(enumerate(mu)), dict(enumerate(mu))
    one = (jnp.ones_like(mu[0][0]), jnp.zeros_like(mu[0][0]))
    p, q = [one], [one]
    x = []
    for k in range(4):
        inverse = dd_inverse(t[k + 1])
        alpha = dd_mul(s[k], inverse)
        minus = dd_neg(alpha)
        x = [dd_add(x[i], dd_mul(alpha, q[i])) if i < len(x) else dd_mul(alpha, q[i]) for i in range(k + 1)]
        moved = [dd_mul(minus, c) for c in q]
        p = [p[i] if i == 0 else (dd_add(p[i], moved[i - 1]) if i <= k else moved[i - 1]) for i in range(k + 2)]
        if k < 3:
            last = 6 - k
            s_next = {j: dd_add(s[j], dd_mul(minus, t[j + 1])) for j in range(k + 1, last + 1)}
            beta = dd_mul(dd_neg(s_next[k + 1]), inverse)
            t = {j: dd_add(s_next[j], dd_mul(beta, t[j])) for j in range(k + 2, last + 1)}
            s = s_next
            q = [dd_add(p[i], dd_mul(beta, q[i])) if i <= k else p[i] for i in range(k + 2)]
    return x, p


def tendencies(active, quads):
    east = shift_lanes(active, 1)
    north = shift_rows(active, 1)
    face_e = active * east
    face_n = active * north
    count = face_e + shift_lanes(face_e, -1) + face_n + shift_rows(face_n, -1)
    u, v = quads[2], quads[3]
    flow_e = (0.25 * face_e) * (u + shift_lanes(u, 1))
    flow_n = (0.25 * face_n) * (v + shift_rows(v, 1))
    own = slice(0, 24)
    flow_w = shift_lanes(flow_e, -1)[own]
    flow_s = shift_rows(flow_n, -1)[own]
    flow_e, flow_n = flow_e[own], flow_n[own]
    net = (flow_e - flow_w) + (flow_n - flow_s)
    out = []
    for q in quads:
        q = active * q
        qe, qw, qn, qs = shift_lanes(q, 1), shift_lanes(q, -1), shift_rows(q, 1), shift_rows(q, -1)
        lap = active * ((qe + qw) + (qn + qs)) - count * q
        around = (shift_lanes(lap, 1) + shift_lanes(lap, -1)) + (shift_rows(lap, 1) + shift_rows(lap, -1))
        flux = (net * q[own] + flow_e * qe[own]) + (flow_n * qn[own] - flow_w * qw[own]) - flow_s * qs[own]
        out.append(VISC * (count[own] * lap[own] - active[own] * around[own]) - flux)
    return out


def make_kernel(nx, ny, nlat, levels):
    nplane = nx * ny
    nline = CORES * nlat
    half = levels // 2
    groups = -(-levels // GROUP)
    entries = levels + groups
    def kernel(forcing_hbm, sea_hbm, count_hbm, state_hbm, x_ref, r_ref, tend,
               forcing, sea, count, state, surf, surf_ew, surf_ns, edges, edges_in, rows_up, rows_down,
               rows_in, corners_in, edge_out, partial, gather_a, mid, gather_b,
               in_sem, send_sem, recv_sem, send_a, recv_a, send_b, recv_b):
        x, y = lax.axis_index("x"), lax.axis_index("y")
        core, lat = lax.axis_index("core"), lax.axis_index("lat")

        small = [pltpu.make_async_copy(a, b, in_sem.at[i]) for i, (a, b) in
                 enumerate(((forcing_hbm, forcing), (sea_hbm, sea), (count_hbm, count)))]
        large = [pltpu.make_async_copy(state_hbm.at[f], state.at[f], in_sem.at[3 + f]) for f in range(4)]
        for copy in small + large:
            copy.start()

        flip = 1 - core
        y_east, y_west = y + core, y + ny - flip
        place = {
            1: (lax.rem(x + lax.div(y_east, ny), nx), lax.rem(y_east, ny), flip),
            -1: (lax.rem(x + nx - 1 + lax.div(y_west, ny), nx), lax.rem(y_west, ny), flip),
            0: (x, y, core),
        }
        row = {1: lax.rem(lat + 1, nlat), -1: lax.rem(lat + nlat - 1, nlat), 0: lat}
        near = [(*place[dx], row[dy]) for dx, dy in DIRS]

        def hops(step, size):
            return min(step, size - step)

        plane_steps = sorted(((i, j) for i in range(nx) for j in range(ny) if i or j),
                             key=lambda p: -hops(p[0], nx) - hops(p[1], ny))
        xs = [x] + [lax.rem(x + i, nx) for i in range(1, nx)]
        ys = [y] + [lax.rem(y + j, ny) for j in range(1, ny)]
        plane_peer = [(xs[i], ys[j], core, lat) for i, j in plane_steps]
        line_steps = sorted(((c, j) for c in range(CORES) for j in range(nlat) if c or j),
                            key=lambda p: -hops(p[1], nlat))
        lats = [lat] + [lax.rem(lat + j, nlat) for j in range(1, nlat)]
        line_peer = [(x, y, (core, flip)[c], lats[j]) for c, j in line_steps]
        barrier = pltpu.get_barrier_semaphore()
        far = [p for pair in zip(plane_peer, line_peer) for p in pair]
        peers = far + near[4:] + near[:4] if nplane == nline else plane_peer + line_peer + near
        for peer in peers:
            pl.semaphore_signal(barrier, inc=1, device_id=peer, device_id_type=MESH)

        lane = iota((8, 128), 1)
        sub = iota((8, 128), 0)

        for copy in small:
            copy.wait()
        wet = sea[...] * count[...]
        for t in range(3):
            rows = slice(8 * t, 8 * t + 8)
            surf[t, 0] = wet[rows].astype(F32)
            surf[t, 1] = (sea[rows].astype(F32) * forcing[rows]) * 65536.0

        partial[...] = jnp.zeros_like(partial)
        mid[...] = jnp.zeros_like(mid)
        for copy in large:
            copy.wait()

        lane24 = iota((24, 128), 1)

        def pack_edges(f, carry):
            for g in range(groups):
                packed = jnp.zeros((24, 128), F32)
                for i in range(min(GROUP, levels - g * GROUP)):
                    moved = pltpu.roll(state[f, g * GROUP + i], (4 + 8 * i) % 128, 1)
                    packed = jnp.where(lane24 // 8 == i, moved, packed)
                edges[f, g] = packed
            return carry

        lax.fori_loop(0, 4, pack_edges, 0)

        def packed_rows(tile_of):
            up, down = None, None
            for f in range(4):
                top = pltpu.roll(tile_of(f, slice(16, 24)), (2 * f + 2) % 8, 0)
                low = tile_of(f, slice(0, 8))
                low = pltpu.roll(low, 2 * f, 0) if f else low
                up = top if f == 0 else jnp.where(sub // 2 == f, top, up)
                down = low if f == 0 else jnp.where(sub // 2 == f, low, down)
            return up, down

        def pack_rows(k, carry):
            up, down = packed_rows(lambda f, rows: state[f, k, rows])
            rows_up[k] = up
            rows_down[k] = down
            return carry

        lax.fori_loop(0, levels, pack_rows, 0)
        for g in range(groups):
            up, down = packed_rows(lambda f, rows: edges[f, g, rows])
            rows_up[levels + g] = up
            rows_down[levels + g] = down

        pl.semaphore_wait(barrier, len(peers))

        def surf_slot(d):
            return surf_ew.at[d] if d < 2 else surf_ns.at[d - 2]

        def surf_copy(d):
            source = surf if d < 2 else surf.at[2 if DIRS[d][1] > 0 else 0]
            return pltpu.make_async_remote_copy(source, surf_slot(OPP[d]), send_sem.at[d], recv_sem.at[OPP[d]],
                                                device_id=near[d], device_id_type=MESH)

        def rows_copy(d, part):
            source = rows_up if DIRS[d][1] > 0 else rows_down
            if d < 4:
                target = rows_in.at[OPP[d] - 2]
                span = pl.ds(0, half) if part == 0 else pl.ds(half, entries - half)
                source, target = source.at[span], target.at[span]
            else:
                source, target = source.at[pl.ds(levels, groups)], corners_in.at[OPP[d] - 4]
            sem = 8 + 8 * part
            return pltpu.make_async_remote_copy(source, target, send_sem.at[sem + d], recv_sem.at[sem + OPP[d]],
                                                device_id=near[d], device_id_type=MESH)

        def edge_copy(d):
            return pltpu.make_async_remote_copy(edges, edges_in.at[OPP[d]], send_sem.at[8 + d], recv_sem.at[8 + OPP[d]],
                                                device_id=near[d], device_id_type=MESH)

        surf_copies = [surf_copy(d) for d in (NE, NW, SE, SW, N, S, E, W)]
        first_rows = [rows_copy(d, 0) for d in (N, S)]
        last_rows = [rows_copy(d, 1) for d in (N, S)]
        edge_copies = [edge_copy(d) for d in (E, W)] + [rows_copy(d, 0) for d in (NE, NW, SE, SW)]
        other_copies = first_rows + edge_copies + last_rows
        for copy in surf_copies + other_copies:
            copy.start()
        for copy in surf_copies:
            copy.wait_recv()

        has_north = jnp.where(lat < nlat - 1, 1.0, 0.0).astype(F32)
        has_south = jnp.where(lat > 0, 1.0, 0.0).astype(F32)

        def wide(v):
            own = [surf[t, v] for t in range(3)] + [surf_ns[N - 2, v] * has_north, surf_ns[S - 2, v] * has_south]
            side = [jnp.where(lane < 64, surf_ew[E, t, v], surf_ew[W, t, v]) for t in range(3)]
            side.append(jnp.where(lane < 64, surf_ns[NE - 2, v], surf_ns[NW - 2, v]) * has_north)
            side.append(jnp.where(lane < 64, surf_ns[SE - 2, v], surf_ns[SW - 2, v]) * has_south)
            return jnp.concatenate(own, 0), jnp.concatenate(side, 0)

        lane40 = iota((40, 128), 1)

        def to_east(pair):
            a, b = shift_lanes(pair[0], 1), shift_lanes(pair[1], 1)
            return jnp.where(lane40 == 127, b, a), jnp.where(lane40 == 127, a, b)

        def to_west(pair):
            a, b = shift_lanes(pair[0], -1), shift_lanes(pair[1], -1)
            return jnp.where(lane40 == 0, b, a), jnp.where(lane40 == 0, a, b)

        def to_north(pair):
            return shift_rows(pair[0], 1), shift_rows(pair[1], 1)

        def to_south(pair):
            return shift_rows(pair[0], -1), shift_rows(pair[1], -1)

        moves = (to_east, to_west, to_north, to_south)
        depth = wide(0)
        force = wide(1)
        moved = [move(depth) for move in moves]
        faces = [[jnp.minimum(depth[t], m[t]) for m in moved] for t in range(2)]
        diag = [2.0 + ((faces[t][0] + faces[t][1]) + (faces[t][2] + faces[t][3])) for t in range(2)]
        inverse = [1.0 / diag[t] for t in range(2)]

        def over_diag(hi, lo, t):
            q = hi * inverse[t]
            a, b = split(q)
            rest = ((hi - diag[t] * a) - diag[t] * b) + lo
            return q, rest * inverse[t]

        vectors = [[quick(*over_diag(force[t], jnp.zeros_like(force[t]), t)) for t in range(2)]]
        for k in range(4):
            last = vectors[-1]
            high = [move((last[0][0], last[1][0])) for move in moves]
            low = [move((last[0][1], last[1][1])) for move in moves]
            following = []
            for t in range(2):
                if k == 3 and t == 1:
                    continue
                terms = [int_prod(faces[t][i], high[i][t]) for i in range(4)]
                fine = [faces[t][i] * low[i][t] + terms[i][1] for i in range(4)]
                s0, e0 = two_sum(terms[0][0], terms[1][0])
                s1, e1 = two_sum(terms[2][0], terms[3][0])
                s, e2 = two_sum(s0, s1)
                rest = ((e0 + e1) + e2) + ((fine[0] + fine[1]) + (fine[2] + fine[3]))
                q, q_low = over_diag(s, rest, t)
                s, e = two_sum(last[t][0], -q)
                following.append(quick(s, e + (last[t][1] - q_low)))
            vectors.append(following)
        own_vectors = [(v[0][0][:24], v[0][1][:24]) for v in vectors]
        own_diag = diag[0][:24]

        sums = []
        for n in range(8):
            a, b = own_vectors[n // 2], own_vectors[n - n // 2]
            p, e = int_prod(own_diag, a[0])
            product = dd_mul(quick(p, e + own_diag * a[1]), b)
            tiles = [(product[0][8 * i:8 * i + 8], product[1][8 * i:8 * i + 8]) for i in range(3)]
            sums.append(dd_add(dd_add(tiles[0], tiles[1]), tiles[2]))

        def fold(a, b, near_mask, step):
            def one(i):
                x, y = a[i], b[i]
                far = jnp.where(near_mask, pltpu.roll(x, 8 - step, 0), pltpu.roll(y, step, 0))
                return jnp.where(near_mask, x, y), far
            kept, far = zip(*(one(i) for i in range(2)))
            return dd_add(kept, far)

        level = [fold(sums[2 * i], sums[2 * i + 1], sub < 4, 4) for i in range(4)]
        level = [fold(level[2 * i], level[2 * i + 1], sub % 4 < 2, 2) for i in range(2)]
        level = fold(level[0], level[1], sub % 2 < 1, 1)
        parts = [x.T for x in level]
        parts = [tuple(p[8 * i:8 * i + 8] for p in parts) for i in range(16)]
        while len(parts) > 1:
            parts = [dd_add(parts[i], parts[i + 1]) for i in range(0, len(parts), 2)]
        level = parts[0]
        for step in (4, 2, 1):
            level = dd_add(tuple(p[:step] for p in level), tuple(p[step:2 * step] for p in level))
        partial[0:1, 0:8] = level[0]
        partial[1:2, 0:8] = level[1]

        copies_a = [pltpu.make_async_remote_copy(partial, gather_a.at[j], send_a.at[j], recv_a.at[j],
                                                 device_id=plane_peer[j], device_id_type=MESH)
                    for j in range(nplane - 1)]
        for copy in copies_a:
            copy.start()

        def total(own, others, number):
            parts = [(own[0:1], own[1:2])] + [(others[j, 0:1], others[j, 1:2]) for j in range(number)]
            while len(parts) > 1:
                parts = [dd_add(parts[i], parts[i + 1]) if i + 1 < len(parts) else parts[i]
                         for i in range(0, len(parts), 2)]
            return parts[0]

        for copy in first_rows:
            copy.wait_recv()
        count_own = jnp.concatenate([depth[0][:24], jnp.where(sub < 4, depth[0][24:32], depth[0][32:40])], 0)
        count_side = jnp.concatenate([depth[1][:24], jnp.where(sub < 4, depth[1][24:32], depth[1][32:40])], 0)

        def with_rows(f, block, north, south):
            up = pltpu.roll(north, (8 - 2 * f) % 8, 0) if f else north
            down = pltpu.roll(south, 6 - 2 * f, 0) if f < 3 else south
            return jnp.concatenate([block, jnp.where(sub < 4, up, down)], 0)

        def main(k):
            active = jnp.where(count_own > k.astype(F32), 1.0, 0.0)
            north, south = rows_in[N - 2, k], rows_in[S - 2, k]
            quads = [with_rows(f, state[f, k], north, south) for f in range(4)]
            for f, value in enumerate(tendencies(active, quads)):
                tend[f, k] = value

        def unrolled(body, first, last, by):
            def step(i, carry):
                for j in range(by):
                    body(first + i * by + j)
                return carry
            lax.fori_loop(0, (last - first) // by, step, 0)

        unrolled(main, 0, half, UNROLL)

        for copy in copies_a:
            copy.wait_recv()
        hi, lo = total(partial, gather_a, nplane - 1)
        mid[0:1] = hi
        mid[1:2] = lo
        copies_b = [pltpu.make_async_remote_copy(mid, gather_b.at[j], send_b.at[j], recv_b.at[j],
                                                 device_id=line_peer[j], device_id_type=MESH)
                    for j in range(nline - 1)]
        for copy in copies_b:
            copy.start()

        for copy in last_rows:
            copy.wait_recv()
        unrolled(main, half, levels, UNROLL)
        for copy in edge_copies:
            copy.wait_recv()
        lane32 = iota((32, 128), 1)
        left32, left24, left8 = lane32 % 8 < 4, lane24 % 8 < 4, lane % 8 < 4

        def spread(first, second):
            x = jnp.where(lane32 < 8, jnp.where(lane32 < 4, pltpu.roll(first, 4, 1), pltpu.roll(second, 4, 1)), 0.0)
            for step in (8, 16, 32, 64):
                x = x + pltpu.roll(x, step, 1)
            return x

        count_w = spread(count_side, count_own)
        count_e = spread(count_own, count_side)

        for g in range(groups):
            kvec = (lane32 // 8 + g * GROUP).astype(F32)
            own_n, own_s = rows_in[N - 2, levels + g], rows_in[S - 2, levels + g]
            results = []
            for side in (W, E):
                if side == W:
                    counts = count_w
                    north = jnp.where(left8, corners_in[NW - 4, g], own_n)
                    south = jnp.where(left8, corners_in[SW - 4, g], own_s)
                    blocks = [jnp.where(left24, edges_in[W, f, g], edges[f, g]) for f in range(4)]
                else:
                    counts = count_e
                    north = jnp.where(left8, own_n, corners_in[NE - 4, g])
                    south = jnp.where(left8, own_s, corners_in[SE - 4, g])
                    blocks = [jnp.where(left24, edges[f, g], edges_in[E, f, g]) for f in range(4)]
                active = jnp.where(counts > kvec, 1.0, 0.0)
                results.append(tendencies(active, [with_rows(f, blocks[f], north, south) for f in range(4)]))
            for f in range(4):
                edge_out[f, g] = jnp.where(left24, results[1][f], results[0][f])

        rim = (lane24 < 2) | (lane24 >= 126)

        def blend(k):
            g = k // GROUP
            back = (128 + 124 - 8 * (k % GROUP)) % 128
            for f in range(4):
                tend[f, k] = jnp.where(rim, pltpu.roll(edge_out[f, g], back, 1), tend[f, k])

        unrolled(blend, 0, levels, 8)

        for copy in copies_b:
            copy.wait_recv()
        level = total(mid, gather_b, nline - 1)

        def scalar(a, n):
            return jnp.broadcast_to(a[0:1, n:n + 1], (8, 128))

        mu = []
        for n in range(8):
            at = 4 * (n % 2) + 2 * (n // 2 % 2) + n // 4
            mu.append((scalar(level[0], at), scalar(level[1], at)))
        x_poly, r_poly = cg_coefficients(mu)
        for t in range(3):
            rows = slice(8 * t, 8 * t + 8)
            basis = [(v[0][rows], v[1][rows]) for v in own_vectors]

            def combined(poly):
                parts = [dd_mul(c, b) for c, b in zip(poly, basis)]
                while len(parts) > 1:
                    parts = [dd_add(parts[i], parts[i + 1]) if i + 1 < len(parts) else parts[i]
                             for i in range(0, len(parts), 2)]
                return parts[0]

            height = combined(x_poly)
            x_ref[rows] = (height[0] + height[1]) * (40.0 / 65536.0)
            rest = combined(r_poly)
            d = own_diag[rows]
            r_ref[rows] = (d * rest[0] + d * rest[1]) * (1.0 / 65536.0)

        for copy in surf_copies + other_copies + copies_a + copies_b:
            copy.wait_send()

    scratch = [
        pltpu.VMEM((24, 128), F32), pltpu.VMEM((24, 128), jnp.int32), pltpu.VMEM((24, 128), jnp.int32),
        pltpu.VMEM((4, levels, 24, 128), F32),
        pltpu.VMEM((3, 2, 8, 128), F32), pltpu.VMEM((2, 3, 2, 8, 128), F32), pltpu.VMEM((6, 2, 8, 128), F32),
        pltpu.VMEM((4, groups, 24, 128), F32), pltpu.VMEM((2, 4, groups, 24, 128), F32),
        pltpu.VMEM((entries, 8, 128), F32), pltpu.VMEM((entries, 8, 128), F32),
        pltpu.VMEM((2, entries, 8, 128), F32), pltpu.VMEM((4, groups, 8, 128), F32),
        pltpu.VMEM((4, groups, 24, 128), F32),
        pltpu.VMEM((2, 128), F32), pltpu.VMEM((nplane - 1, 2, 128), F32),
        pltpu.VMEM((2, 128), F32), pltpu.VMEM((nline - 1, 2, 128), F32),
        pltpu.SemaphoreType.DMA((7,)),
        pltpu.SemaphoreType.DMA((24,)), pltpu.SemaphoreType.DMA((24,)),
        pltpu.SemaphoreType.DMA((nplane - 1,)), pltpu.SemaphoreType.DMA((nplane - 1,)),
        pltpu.SemaphoreType.DMA((nline - 1,)), pltpu.SemaphoreType.DMA((nline - 1,)),
    ]
    return kernel, scratch


def hand_out(x_ref, r_ref, tend_ref, x_out, r_out, tend_out, sem):
    copies = [pltpu.make_async_copy(tend_ref.at[f], tend_out.at[f], sem.at[f]) for f in range(4)]
    copies += [pltpu.make_async_copy(x_ref, x_out, sem.at[4]), pltpu.make_async_copy(r_ref, r_out, sem.at[5])]
    for copy in copies:
        copy.start()
    for copy in copies:
        copy.wait()


def solution(mesh):
    nlon, nlat = mesh.shape["lon"], mesh.shape["lat"]
    nplane = nlon // CORES
    nx = max(n for n in range(1, nplane + 1) if nplane % n == 0 and n * n <= nplane)
    ny = nplane // nx
    finer = Mesh(mesh.devices.reshape(nx, ny, CORES, nlat), ("x", "y", "core", "lat"))

    def per_device(surface_forcing, sea_mask, level_count, state):
        kernel, scratch = make_kernel(nx, ny, nlat, state.shape[1])
        results = pl.pallas_call(
            kernel,
            out_shape=(
                pltpu.VMEM(surface_forcing.shape, F32),
                pltpu.VMEM(surface_forcing.shape, F32),
                pltpu.VMEM(state.shape, F32),
            ),
            in_specs=[pl.BlockSpec(memory_space=pl.ANY)] * 4,
            out_specs=(
                pl.BlockSpec(memory_space=pltpu.VMEM),
                pl.BlockSpec(memory_space=pltpu.VMEM),
                pl.BlockSpec(memory_space=pltpu.VMEM),
            ),
            scratch_shapes=scratch,
            compiler_params=pltpu.CompilerParams(collective_id=0, has_side_effects=True, vmem_limit_bytes=65_030_000),
            name="ocean",
        )(surface_forcing, sea_mask, level_count, state)
        return pl.pallas_call(
            hand_out,
            out_shape=tuple(jax.ShapeDtypeStruct(r.shape, F32) for r in results),
            in_specs=[pl.BlockSpec(memory_space=pltpu.VMEM)] * 3,
            out_specs=[pl.BlockSpec(memory_space=pl.ANY)] * 3,
            scratch_shapes=[pltpu.SemaphoreType.DMA((6,))],
            compiler_params=pltpu.CompilerParams(vmem_limit_bytes=8 * 2**20),
            name="hand_out",
        )(*results)

    flat, deep = P("lat", ("x", "y", "core")), P(None, None, "lat", ("x", "y", "core"))
    return jax.shard_map(
        per_device, mesh=finer, in_specs=(flat, flat, flat, deep), out_specs=(flat, flat, deep), check_vma=False
    )
```

```python
import jax
import jax.numpy as jnp
from jax import lax
from jax.experimental import pallas as pl
from jax.experimental.pallas import tpu as pltpu
from jax.sharding import Mesh
from jax.sharding import PartitionSpec as P

MESH = pl.DeviceIdType.MESH
F32 = jnp.float32
CORES = 2
GROUP = 16
VISC = 0.02
UNROLL = 2
FINISH = 8
DIRS = ((1, 0), (-1, 0), (0, 1), (0, -1), (1, 1), (-1, -1), (1, -1), (-1, 1))
OPP = (1, 0, 3, 2, 5, 4, 7, 6)
E, W, N, S, NE, SW, SE, NW = range(8)


def two_sum(a, b):
    s = a + b
    t = s - a
    return s, (a - (s - t)) + (b - t)


def quick(a, b):
    s = a + b
    return s, b - (s - a)


def split(a):
    t = 4097.0 * a
    h = t - (t - a)
    return h, a - h


def two_prod(a, b):
    p = a * b
    ah, al = split(a)
    bh, bl = split(b)
    return p, ((ah * bh - p) + ah * bl + al * bh) + al * bl


def short(hi, lo):
    t = 257.0 * hi
    h = t - (t - hi)
    return h, (hi - h) + lo


def dd_add(a, b):
    s, e = two_sum(a[0], b[0])
    return quick(s, e + (a[1] + b[1]))


def dd_mul(a, b):
    p, e = two_prod(a[0], b[0])
    return quick(p, e + (a[0] * b[1] + a[1] * b[0]))


def dd_neg(a):
    return -a[0], -a[1]


def dd_inverse(b):
    r = 1.0 / b[0]
    p, e = two_prod(r, b[0])
    rest = ((1.0 - p) - e) - r * b[1]
    return quick(r, rest * r)


def iota(shape, dim):
    return lax.broadcasted_iota(jnp.int32, shape, dim)


def shift_rows(x, step):
    return pltpu.roll(x, (-step) % x.shape[0], 0)


def shift_lanes(x, step):
    return pltpu.roll(x, (-step) % 128, 1)


def cg_coefficients(mu):
    s, t = dict(enumerate(mu)), dict(enumerate(mu))
    one = (jnp.ones_like(mu[0][0]), jnp.zeros_like(mu[0][0]))
    p, q = [one], [one]
    x = []
    for k in range(4):
        inverse = dd_inverse(t[k + 1])
        alpha = dd_mul(s[k], inverse)
        minus = dd_neg(alpha)
        x = [dd_add(x[i], dd_mul(alpha, q[i])) if i < len(x) else dd_mul(alpha, q[i]) for i in range(k + 1)]
        moved = [dd_mul(minus, c) for c in q]
        p = [p[i] if i == 0 else (dd_add(p[i], moved[i - 1]) if i <= k else moved[i - 1]) for i in range(k + 2)]
        if k < 3:
            last = 6 - k
            s_next = {j: dd_add(s[j], dd_mul(minus, t[j + 1])) for j in range(k + 1, last + 1)}
            beta = dd_mul(dd_neg(s_next[k + 1]), inverse)
            t = {j: dd_add(s_next[j], dd_mul(beta, t[j])) for j in range(k + 2, last + 1)}
            s = s_next
            q = [dd_add(p[i], dd_mul(beta, q[i])) if i <= k else p[i] for i in range(k + 2)]
    return x, p


def first_pass(active, quads, masked, laps, weight):
    own = slice(0, 24)
    face_e, face_w = active * shift_lanes(active, 1), active * shift_lanes(active, -1)
    face_n, face_s = active * shift_rows(active, 1), active * shift_rows(active, -1)
    count = (face_e + face_w) + (face_n + face_s)
    weight[...] = VISC * active[own]
    visc_count = VISC * count[own]
    near = []
    for f, q in enumerate(quads):
        q = active * q
        masked[f, 0:8] = q[24:32]
        masked[f, 8:40] = q
        masked[f, 40:48] = q[0:8]
        near.append((q, shift_lanes(q, 1), shift_lanes(q, -1)))
    u, ue, uw = (x[own] for x in near[2])
    v = near[3][0][own]
    flow_e = (0.25 * face_e[own]) * (u + ue)
    flow_w = (0.25 * face_w[own]) * (u + uw)
    flow_n = (0.25 * face_n[own]) * (v + masked[3, 9:33])
    flow_s = (0.25 * face_s[own]) * (v + masked[3, 7:31])
    net = (flow_e - flow_w) + (flow_n - flow_s)
    out = []
    for f, (q, qe, qw) in enumerate(near):
        qn, qs = masked[f, 9:41], masked[f, 7:39]
        lap = active * ((qe + qw) + (qn + qs)) - count * q
        laps[f, 0:8] = lap[24:32]
        laps[f, 8:40] = lap
        flux = (net * q[own] + flow_e * qe[own]) + (flow_n * qn[own] - flow_w * qw[own]) - flow_s * qs[own]
        out.append(visc_count * lap[own] - flux)
    return out


def second_pass(f, laps, weight):
    lap = laps[f, 8:32]
    around = (shift_lanes(lap, 1) + shift_lanes(lap, -1)) + (laps[f, 9:33] + laps[f, 7:31])
    return weight[...] * around


def make_kernel(nx, ny, nlat, levels):
    nplane = nx * ny
    nline = CORES * nlat
    half = 3 * levels // 5
    groups = -(-levels // GROUP)
    entries = levels + groups
    def kernel(forcing_hbm, sea_hbm, count_hbm, state_hbm, x_ref, r_ref, tend,
               forcing, sea, count, state, surf, surf_in, edges, edges_in, rows_up, rows_down,
               rows_a, rows_b, corners_in, counts, masked, laps, weight, edge_out, partial, gather_a, mid, gather_b, in_sem, send_sem, recv_sem, ready):
        x, y = lax.axis_index("x"), lax.axis_index("y")
        core, lat = lax.axis_index("core"), lax.axis_index("lat")

        small = [pltpu.make_async_copy(a, b, in_sem.at[i]) for i, (a, b) in
                 enumerate(((forcing_hbm, forcing), (sea_hbm, sea), (count_hbm, count)))]
        large = [pltpu.make_async_copy(state_hbm.at[pl.ds(2 * f, 2)], state.at[pl.ds(2 * f, 2)], in_sem.at[3 + f])
                 for f in range(2)]
        for copy in small + large:
            copy.start()

        flip = 1 - core
        y_east, y_west = y + core, y + ny - flip
        place = {
            1: (lax.rem(x + lax.div(y_east, ny), nx), lax.rem(y_east, ny), flip),
            -1: (lax.rem(x + nx - 1 + lax.div(y_west, ny), nx), lax.rem(y_west, ny), flip),
            0: (x, y, core),
        }
        row = {1: lax.rem(lat + 1, nlat), -1: lax.rem(lat + nlat - 1, nlat), 0: lat}
        near = [(*place[dx], row[dy]) for dx, dy in DIRS]

        def hops(step, size):
            return min(step, size - step)

        plane_steps = sorted(((i, j) for i in range(nx) for j in range(ny) if i or j),
                             key=lambda p: -hops(p[0], nx) - hops(p[1], ny))
        xs = [x] + [lax.rem(x + i, nx) for i in range(1, nx)]
        ys = [y] + [lax.rem(y + j, ny) for j in range(1, ny)]
        plane_peer = [(xs[i], ys[j], core, lat) for i, j in plane_steps]
        line_steps = sorted(((c, j) for c in range(CORES) for j in range(nlat) if c or j),
                            key=lambda p: -hops(p[1], nlat))
        lats = [lat] + [lax.rem(lat + j, nlat) for j in range(1, nlat)]
        line_peer = [(x, y, (core, flip)[c], lats[j]) for c, j in line_steps]
        barrier = pltpu.get_barrier_semaphore()
        column = [(x, p, core, lat) for p in ys[1:]]
        rows = [(p, y, core, lat) for p in xs[1:]]
        along = [(x, y, c, lax.rem(lat + j, nlat)) for j in (2, nlat - 2, 1, nlat - 1) for c in (core, flip)]
        relay = column + [(x, y, core, lax.rem(lat + j, nlat)) for j in (2, nlat - 2)]
        peers = near[4:] + along[:4] + column + rows + near[:4] + along[4:] + [(x, y, flip, lat)]
        for peer in peers:
            pl.semaphore_signal(barrier, inc=1, device_id=peer, device_id_type=MESH)

        lane = iota((8, 128), 1)
        sub = iota((8, 128), 0)

        for copy in small:
            copy.wait()
        wet = sea[...] * count[...]
        for t in range(3):
            rows = slice(8 * t, 8 * t + 8)
            surf[t, 0] = wet[rows].astype(F32)
            surf[t, 1] = (sea[rows].astype(F32) * forcing[rows]) * 65536.0

        partial[...] = jnp.zeros_like(partial)
        mid[...] = jnp.zeros_like(mid)
        pl.semaphore_wait(barrier, len(peers))

        def remote(source, target, i, peer):
            return pltpu.make_async_remote_copy(source, target, send_sem.at[i], recv_sem.at[i],
                                                device_id=peer, device_id_type=MESH)

        def surf_slot(d):
            return surf_in.at[pl.ds(3 * d, 3)] if d < 2 else surf_in.at[pl.ds(4 + d, 1)]

        def surf_copy(d):
            source = surf if d < 2 else surf.at[pl.ds(2 if DIRS[d][1] > 0 else 0, 1)]
            return remote(source, surf_slot(OPP[d]), 0, near[d])

        def rows_copy(d, part):
            source = rows_up if DIRS[d][1] > 0 else rows_down
            span = pl.ds(0, half) if part == 0 else pl.ds(half, entries - half)
            return remote(source.at[span], (rows_a, rows_b)[part].at[OPP[d] - 2], 1 + part, near[d])

        def corner_copy(d):
            source = rows_up if DIRS[d][1] > 0 else rows_down
            return remote(source.at[pl.ds(levels, groups)], corners_in.at[OPP[d] - 4], 3, near[d])

        def edge_copy(d):
            return remote(edges, edges_in.at[OPP[d]], 4, near[d])

        landing = (surf_in, rows_a, rows_b, corners_in, edges_in, gather_a, gather_b)

        def wait_all(sem, i):
            pltpu.make_async_copy(landing[i], landing[i], sem.at[i]).wait()

        for d in (NE, NW, SE, SW, N, S, E, W):
            surf_copy(d).start()
        for peer in relay:
            pl.semaphore_signal(ready, inc=1, device_id=peer, device_id_type=MESH)
        for copy in large:
            copy.wait()

        lane24 = iota((24, 128), 1)

        def pack_edges(f, carry):
            for g in range(groups):
                packed = jnp.zeros((24, 128), F32)
                for i in range(min(GROUP, levels - g * GROUP)):
                    moved = pltpu.roll(state[f, g * GROUP + i], (4 + 8 * i) % 128, 1)
                    packed = jnp.where(lane24 // 8 == i, moved, packed)
                edges[f, g] = packed
            return carry


        def packed_rows(tile_of):
            up, down = None, None
            for f in range(4):
                top = pltpu.roll(tile_of(f, slice(16, 24)), (2 * f + 2) % 8, 0)
                low = tile_of(f, slice(0, 8))
                low = pltpu.roll(low, 2 * f, 0) if f else low
                up = top if f == 0 else jnp.where(sub // 2 == f, top, up)
                down = low if f == 0 else jnp.where(sub // 2 == f, low, down)
            return up, down

        def pack_rows(k, carry):
            up, down = packed_rows(lambda f, rows: state[f, k, rows])
            rows_up[k] = up
            rows_down[k] = down
            return carry

        lax.fori_loop(0, levels, pack_rows, 0)
        for d in (N, S):
            rows_copy(d, 0).start()
        lax.fori_loop(0, 4, pack_edges, 0)
        for g in range(groups):
            up, down = packed_rows(lambda f, rows: edges[f, g, rows])
            rows_up[levels + g] = up
            rows_down[levels + g] = down

        for d in (E, W):
            edge_copy(d).start()
        for d in (NE, NW, SE, SW):
            corner_copy(d).start()
        for d in (N, S):
            rows_copy(d, 1).start()
        wait_all(recv_sem, 0)

        has_north = jnp.where(lat < nlat - 1, 1.0, 0.0).astype(F32)
        has_south = jnp.where(lat > 0, 1.0, 0.0).astype(F32)

        def wide(v):
            own = [surf[t, v] for t in range(3)] + [surf_in[4 + N, v] * has_north, surf_in[4 + S, v] * has_south]
            side = [jnp.where(lane < 64, surf_in[t, v], surf_in[3 + t, v]) for t in range(3)]
            side.append(jnp.where(lane < 64, surf_in[4 + NE, v], surf_in[4 + NW, v]) * has_north)
            side.append(jnp.where(lane < 64, surf_in[4 + SE, v], surf_in[4 + SW, v]) * has_south)
            return jnp.concatenate(own, 0), jnp.concatenate(side, 0)

        lane40 = iota((40, 128), 1)

        def to_east(pair):
            a, b = shift_lanes(pair[0], 1), shift_lanes(pair[1], 1)
            return jnp.where(lane40 == 127, b, a), jnp.where(lane40 == 127, a, b)

        def to_west(pair):
            a, b = shift_lanes(pair[0], -1), shift_lanes(pair[1], -1)
            return jnp.where(lane40 == 0, b, a), jnp.where(lane40 == 0, a, b)

        def to_north(pair):
            return shift_rows(pair[0], 1), shift_rows(pair[1], 1)

        def to_south(pair):
            return shift_rows(pair[0], -1), shift_rows(pair[1], -1)

        moves = (to_east, to_west, to_north, to_south)
        depth = wide(0)
        force = wide(1)
        moved = [move(depth) for move in moves]
        faces = [[jnp.minimum(depth[t], m[t]) for m in moved] for t in range(2)]
        diag = [2.0 + ((faces[t][0] + faces[t][1]) + (faces[t][2] + faces[t][3])) for t in range(2)]
        inverse = [1.0 / diag[t] for t in range(2)]

        def over_diag(hi, lo, t):
            q, rest = short(hi * inverse[t], 0.0)
            return q, ((hi - diag[t] * q) + lo) * inverse[t]

        vectors = [[short(*over_diag(force[t], 0.0, t)) for t in range(2)]]
        for k in range(4):
            last = vectors[-1]
            high = [move((last[0][0], last[1][0])) for move in moves]
            low = [move((last[0][1], last[1][1])) for move in moves]
            following = []
            for t in range(2):
                if k == 3 and t == 1:
                    continue
                terms = [faces[t][i] * high[i][t] for i in range(4)]
                fine = [faces[t][i] * low[i][t] for i in range(4)]
                s0, e0 = two_sum(terms[0], terms[1])
                s1, e1 = two_sum(terms[2], terms[3])
                s, e2 = two_sum(s0, s1)
                rest = ((e0 + e1) + e2) + ((fine[0] + fine[1]) + (fine[2] + fine[3]))
                q, q_low = over_diag(s, rest, t)
                s, e = two_sum(last[t][0], -q)
                following.append(short(s, e + (last[t][1] - q_low)))
            vectors.append(following)
        own_vectors = [quick(v[0][0][:24], v[0][1][:24]) for v in vectors]
        own_diag = diag[0][:24]
        weighted = [quick(own_diag * v[0][0][:24], own_diag * v[0][1][:24]) for v in vectors[:4]]

        sums = []
        for n in range(8):
            product = dd_mul(weighted[n // 2], own_vectors[n - n // 2])
            tiles = [(product[0][8 * i:8 * i + 8], product[1][8 * i:8 * i + 8]) for i in range(3)]
            sums.append(dd_add(dd_add(tiles[0], tiles[1]), tiles[2]))

        def fold(a, b, near_mask, step):
            def one(i):
                x, y = a[i], b[i]
                far = jnp.where(near_mask, pltpu.roll(x, 8 - step, 0), pltpu.roll(y, step, 0))
                return jnp.where(near_mask, x, y), far
            kept, far = zip(*(one(i) for i in range(2)))
            return dd_add(kept, far)

        level = [fold(sums[2 * i], sums[2 * i + 1], sub < 4, 4) for i in range(4)]
        level = [fold(level[2 * i], level[2 * i + 1], sub % 4 < 2, 2) for i in range(2)]
        level = fold(level[0], level[1], sub % 2 < 1, 1)
        parts = [x.T for x in level]
        parts = [tuple(p[8 * i:8 * i + 8] for p in parts) for i in range(16)]
        while len(parts) > 1:
            parts = [dd_add(parts[i], parts[i + 1]) for i in range(0, len(parts), 2)]
        level = parts[0]
        for step in (4, 2, 1):
            level = dd_add(tuple(p[:step] for p in level), tuple(p[step:2 * step] for p in level))
        partial[0:1, 0:8] = level[0]
        partial[1:2, 0:8] = level[1]

        pl.semaphore_wait(ready, len(relay))
        for j, peer in enumerate(plane_peer):
            remote(partial, gather_a.at[j], 5, peer).start()

        def total(own, others, number):
            parts = [(own[0:1], own[1:2])] + [(others[j, 0:1], others[j, 1:2]) for j in range(number)]
            while len(parts) > 1:
                parts = [dd_add(parts[i], parts[i + 1]) if i + 1 < len(parts) else parts[i]
                         for i in range(0, len(parts), 2)]
            return parts[0]

        wait_all(recv_sem, 1)
        count_own = jnp.concatenate([depth[0][:24], jnp.where(sub < 4, depth[0][24:32], depth[0][32:40])], 0)
        count_side = jnp.concatenate([depth[1][:24], jnp.where(sub < 4, depth[1][24:32], depth[1][32:40])], 0)

        def with_rows(f, block, north, south):
            up = pltpu.roll(north, (8 - 2 * f) % 8, 0) if f else north
            down = pltpu.roll(south, 6 - 2 * f, 0) if f < 3 else south
            return jnp.concatenate([block, jnp.where(sub < 4, up, down)], 0)

        def main(k, slot, rows_in, base):
            active = jnp.where(count_own > k.astype(F32), 1.0, 0.0)
            north, south = rows_in[N - 2, k - base], rows_in[S - 2, k - base]
            quads = [with_rows(f, state[f, k], north, south) for f in range(4)]
            for f, value in enumerate(first_pass(active, quads, masked.at[slot], laps.at[k - base], weight.at[k - base])):
                tend[f, k] = value

        def finish(k, base):
            for f in range(4):
                tend[f, k] = tend[f, k] - second_pass(f, laps.at[k - base], weight.at[k - base])

        def unrolled(body, first, last, by):
            def step(i, carry):
                for j in range(by):
                    body(first + i * by + j, j)
                return carry
            lax.fori_loop(0, (last - first) // by, step, 0)

        unrolled(lambda k, slot: main(k, slot, rows_a, 0), 0, half, UNROLL)
        unrolled(lambda k, slot: finish(k, 0), 0, half, FINISH)

        lane32 = iota((32, 128), 1)

        def spread(first, second):
            x = jnp.where(lane32 < 8, jnp.where(lane32 < 4, pltpu.roll(first, 4, 1), pltpu.roll(second, 4, 1)), 0.0)
            for step in (8, 16, 32, 64):
                x = x + pltpu.roll(x, step, 1)
            return x

        counts[0] = spread(count_side, count_own)
        counts[1] = spread(count_own, count_side)

        wait_all(recv_sem, 5)
        hi, lo = total(partial, gather_a, nplane - 1)
        mid[0:1] = hi
        mid[1:2] = lo
        for j, peer in enumerate(line_peer):
            remote(mid, gather_b.at[j], 6, peer).start()

        wait_all(recv_sem, 2)
        unrolled(lambda k, slot: main(k, slot, rows_b, half), half, levels, UNROLL)
        unrolled(lambda k, slot: finish(k, half), half, levels, FINISH)
        wait_all(recv_sem, 3)
        wait_all(recv_sem, 4)
        left24, left8 = lane24 % 8 < 4, lane % 8 < 4

        def edge_active(side, g):
            return jnp.where(counts[side] > (lane32 // 8 + g * GROUP).astype(F32), 1.0, 0.0)

        def edge_first(g, side, slot):
            if side == 0:
                north = jnp.where(left8, corners_in[NW - 4, g], rows_b[N - 2, levels - half + g])
                south = jnp.where(left8, corners_in[SW - 4, g], rows_b[S - 2, levels - half + g])
                blocks = [jnp.where(left24, edges_in[W, f, g], edges[f, g]) for f in range(4)]
            else:
                north = jnp.where(left8, rows_b[N - 2, levels - half + g], corners_in[NE - 4, g])
                south = jnp.where(left8, rows_b[S - 2, levels - half + g], corners_in[SE - 4, g])
                blocks = [jnp.where(left24, edges[f, g], edges_in[E, f, g]) for f in range(4)]
            quads = [with_rows(f, blocks[f], north, south) for f in range(4)]
            at = 2 * g + side
            return first_pass(edge_active(side, g), quads, masked.at[slot], laps.at[at], weight.at[at])

        def edge(g):
            west, east = edge_first(g, 0, 0), edge_first(g, 1, 1)
            for f in range(4):
                edge_out[f, g] = jnp.where(left24, east[f], west[f])

        def edge_finish(g):
            for f in range(4):
                west, east = (second_pass(f, laps.at[2 * g + i], weight.at[2 * g + i]) for i in range(2))
                edge_out[f, g] = edge_out[f, g] - jnp.where(left24, east, west)

        unrolled(lambda g, slot: edge(g), 0, groups, 1)
        unrolled(lambda g, slot: edge_finish(g), 0, groups, groups)

        rim = (lane24 < 2) | (lane24 >= 126)

        for k in range(levels):
            g, back = k // GROUP, (252 - 8 * (k % GROUP)) % 128
            for f in range(4):
                tend[f, k] = jnp.where(rim, pltpu.roll(edge_out[f, g], back, 1), tend[f, k])

        wait_all(recv_sem, 6)
        level = total(mid, gather_b, nline - 1)

        def scalar(a, n):
            return jnp.broadcast_to(a[0:1, n:n + 1], (8, 128))

        mu = []
        for n in range(8):
            at = 4 * (n % 2) + 2 * (n // 2 % 2) + n // 4
            mu.append((scalar(level[0], at), scalar(level[1], at)))
        x_poly, r_poly = cg_coefficients(mu)
        for t in range(3):
            rows = slice(8 * t, 8 * t + 8)
            basis = [(v[0][rows], v[1][rows]) for v in own_vectors]

            def combined(poly):
                parts = [dd_mul(c, b) for c, b in zip(poly, basis)]
                while len(parts) > 1:
                    parts = [dd_add(parts[i], parts[i + 1]) if i + 1 < len(parts) else parts[i]
                             for i in range(0, len(parts), 2)]
                return parts[0]

            height = combined(x_poly)
            x_ref[rows] = (height[0] + height[1]) * (40.0 / 65536.0)
            rest = combined(r_poly)
            d = own_diag[rows]
            r_ref[rows] = (d * rest[0] + d * rest[1]) * (1.0 / 65536.0)

        for i in range(7):
            wait_all(send_sem, i)

    scratch = [
        pltpu.VMEM((24, 128), F32), pltpu.VMEM((24, 128), jnp.int32), pltpu.VMEM((24, 128), jnp.int32),
        pltpu.VMEM((4, levels, 24, 128), F32),
        pltpu.VMEM((3, 2, 8, 128), F32), pltpu.VMEM((12, 2, 8, 128), F32),
        pltpu.VMEM((4, groups, 24, 128), F32), pltpu.VMEM((2, 4, groups, 24, 128), F32),
        pltpu.VMEM((entries, 8, 128), F32), pltpu.VMEM((entries, 8, 128), F32),
        pltpu.VMEM((2, half, 8, 128), F32), pltpu.VMEM((2, entries - half, 8, 128), F32),
        pltpu.VMEM((4, groups, 8, 128), F32),
        pltpu.VMEM((2, 32, 128), F32), pltpu.VMEM((UNROLL, 4, 48, 128), F32),
        pltpu.VMEM((half, 4, 40, 128), F32), pltpu.VMEM((half, 24, 128), F32),
        pltpu.VMEM((4, groups, 24, 128), F32),
        pltpu.VMEM((2, 128), F32), pltpu.VMEM((nplane - 1, 2, 128), F32),
        pltpu.VMEM((2, 128), F32), pltpu.VMEM((nline - 1, 2, 128), F32),
        pltpu.SemaphoreType.DMA((5,)), pltpu.SemaphoreType.DMA((7,)), pltpu.SemaphoreType.DMA((7,)),
        pltpu.SemaphoreType.REGULAR,
    ]
    return kernel, scratch


def hand_out(x_ref, r_ref, tend_ref, x_out, r_out, tend_out, sem):
    copies = [pltpu.make_async_copy(tend_ref.at[f], tend_out.at[f], sem.at[f]) for f in range(4)]
    copies += [pltpu.make_async_copy(x_ref, x_out, sem.at[4]), pltpu.make_async_copy(r_ref, r_out, sem.at[5])]
    for copy in copies:
        copy.start()
    for copy in copies:
        copy.wait()


def solution(mesh):
    nlon, nlat = mesh.shape["lon"], mesh.shape["lat"]
    nplane = nlon // CORES
    nx = max(n for n in range(1, nplane + 1) if nplane % n == 0 and n * n <= nplane)
    ny = nplane // nx
    finer = Mesh(mesh.devices.reshape(nx, ny, CORES, nlat), ("x", "y", "core", "lat"))

    def per_device(surface_forcing, sea_mask, level_count, state):
        kernel, scratch = make_kernel(nx, ny, nlat, state.shape[1])
        results = pl.pallas_call(
            kernel,
            out_shape=(
                pltpu.VMEM(surface_forcing.shape, F32),
                pltpu.VMEM(surface_forcing.shape, F32),
                pltpu.VMEM(state.shape, F32),
            ),
            in_specs=[pl.BlockSpec(memory_space=pl.ANY)] * 4,
            out_specs=(
                pl.BlockSpec(memory_space=pltpu.VMEM),
                pl.BlockSpec(memory_space=pltpu.VMEM),
                pl.BlockSpec(memory_space=pltpu.VMEM),
            ),
            scratch_shapes=scratch,
            compiler_params=pltpu.CompilerParams(collective_id=0, has_side_effects=True, vmem_limit_bytes=65_030_000),
            name="ocean",
        )(surface_forcing, sea_mask, level_count, state)
        return pl.pallas_call(
            hand_out,
            out_shape=tuple(jax.ShapeDtypeStruct(r.shape, F32) for r in results),
            in_specs=[pl.BlockSpec(memory_space=pltpu.VMEM)] * 3,
            out_specs=[pl.BlockSpec(memory_space=pl.ANY)] * 3,
            scratch_shapes=[pltpu.SemaphoreType.DMA((6,))],
            compiler_params=pltpu.CompilerParams(vmem_limit_bytes=8 * 2**20),
            name="hand_out",
        )(*results)

    flat, deep = P("lat", ("x", "y", "core")), P(None, None, "lat", ("x", "y", "core"))
    return jax.shard_map(
        per_device, mesh=finer, in_specs=(flat, flat, flat, deep), out_specs=(flat, flat, deep), check_vma=False
    )
```

```python
import jax
import jax.numpy as jnp
from jax import lax
from jax.experimental import pallas as pl
from jax.experimental.pallas import tpu as pltpu
from jax.sharding import Mesh
from jax.sharding import PartitionSpec as P

MESH = pl.DeviceIdType.MESH
F32 = jnp.float32
CORES = 2
GROUP = 16
VISC = 0.02
HALO = 5
UNROLL = 2
FINISH = 8
DIRS = ((1, 0), (-1, 0), (0, 1), (0, -1), (1, 1), (-1, -1), (1, -1), (-1, 1))
OPP = (1, 0, 3, 2, 5, 4, 7, 6)
E, W, N, S, NE, SW, SE, NW = range(8)


def two_sum(a, b):
    s = a + b
    t = s - a
    return s, (a - (s - t)) + (b - t)


def quick(a, b):
    s = a + b
    return s, b - (s - a)


def split(a):
    t = 4097.0 * a
    h = t - (t - a)
    return h, a - h


def two_prod(a, b):
    p = a * b
    ah, al = split(a)
    bh, bl = split(b)
    return p, ((ah * bh - p) + ah * bl + al * bh) + al * bl


def short(hi, lo):
    t = 257.0 * hi
    h = t - (t - hi)
    return h, (hi - h) + lo


def dd_add(a, b):
    s, e = two_sum(a[0], b[0])
    return quick(s, e + (a[1] + b[1]))


def dd_mul(a, b):
    p, e = two_prod(a[0], b[0])
    return quick(p, e + (a[0] * b[1] + a[1] * b[0]))


def dd_neg(a):
    return -a[0], -a[1]


def dd_inverse(b):
    r = 1.0 / b[0]
    p, e = two_prod(r, b[0])
    rest = ((1.0 - p) - e) - r * b[1]
    return quick(r, rest * r)


def iota(shape, dim):
    return lax.broadcasted_iota(jnp.int32, shape, dim)


def shift_rows(x, step):
    return pltpu.roll(x, (-step) % x.shape[0], 0)


def shift_lanes(x, step):
    return pltpu.roll(x, (-step) % 128, 1)


def cg_coefficients(mu):
    s, t = dict(enumerate(mu)), dict(enumerate(mu))
    one = (jnp.ones_like(mu[0][0]), jnp.zeros_like(mu[0][0]))
    p, q = [one], [one]
    x = []
    for k in range(4):
        inverse = dd_inverse(t[k + 1])
        alpha = dd_mul(s[k], inverse)
        minus = dd_neg(alpha)
        x = [dd_add(x[i], dd_mul(alpha, q[i])) if i < len(x) else dd_mul(alpha, q[i]) for i in range(k + 1)]
        moved = [dd_mul(minus, c) for c in q]
        p = [p[i] if i == 0 else (dd_add(p[i], moved[i - 1]) if i <= k else moved[i - 1]) for i in range(k + 2)]
        if k < 3:
            last = 6 - k
            s_next = {j: dd_add(s[j], dd_mul(minus, t[j + 1])) for j in range(k + 1, last + 1)}
            beta = dd_mul(dd_neg(s_next[k + 1]), inverse)
            t = {j: dd_add(s_next[j], dd_mul(beta, t[j])) for j in range(k + 2, last + 1)}
            s = s_next
            q = [dd_add(p[i], dd_mul(beta, q[i])) if i <= k else p[i] for i in range(k + 2)]
    return x, p


def first_pass(active, quads, masked, laps, weight):
    own = slice(0, 24)
    face_e, face_w = active * shift_lanes(active, 1), active * shift_lanes(active, -1)
    face_n, face_s = active * shift_rows(active, 1), active * shift_rows(active, -1)
    count = (face_e + face_w) + (face_n + face_s)
    weight[...] = VISC * active[own]
    visc_count = VISC * count[own]
    near = []
    for f, q in enumerate(quads):
        q = active * q
        masked[f, 0:8] = q[24:32]
        masked[f, 8:40] = q
        masked[f, 40:48] = q[0:8]
        near.append((q, shift_lanes(q, 1), shift_lanes(q, -1)))
    u, ue, uw = (x[own] for x in near[2])
    v = near[3][0][own]
    flow_e = (0.25 * face_e[own]) * (u + ue)
    flow_w = (0.25 * face_w[own]) * (u + uw)
    flow_n = (0.25 * face_n[own]) * (v + masked[3, 9:33])
    flow_s = (0.25 * face_s[own]) * (v + masked[3, 7:31])
    net = (flow_e - flow_w) + (flow_n - flow_s)
    out = []
    for f, (q, qe, qw) in enumerate(near):
        qn, qs = masked[f, 9:41], masked[f, 7:39]
        lap = active * ((qe + qw) + (qn + qs)) - count * q
        laps[f, 0:8] = lap[24:32]
        laps[f, 8:40] = lap
        flux = (net * q[own] + flow_e * qe[own]) + (flow_n * qn[own] - flow_w * qw[own]) - flow_s * qs[own]
        out.append(visc_count * lap[own] - flux)
    return out


def second_pass(f, laps, weight):
    lap = laps[f, 8:32]
    around = (shift_lanes(lap, 1) + shift_lanes(lap, -1)) + (laps[f, 9:33] + laps[f, 7:31])
    return weight[...] * around


def make_kernel(nx, ny, nlat, levels):
    nplane = nx * ny
    nline = CORES * nlat
    half = 3 * levels // 5
    groups = -(-levels // GROUP)
    entries = levels + groups
    def kernel(forcing_hbm, sea_hbm, count_hbm, state_hbm, x_ref, r_ref, tend,
               forcing, sea, count, state, surf, surf_in, surf_s, surf_b, edges, edges_in, rows_up, rows_down,
               rows_a, rows_b, corners_in, counts, masked, laps, weight, edge_out, partial, gather_a, mid, gather_b, in_sem, send_sem, recv_sem, ready):
        x, y = lax.axis_index("x"), lax.axis_index("y")
        core, lat = lax.axis_index("core"), lax.axis_index("lat")

        small = [pltpu.make_async_copy(a, b, in_sem.at[i]) for i, (a, b) in
                 enumerate(((forcing_hbm, forcing), (sea_hbm, sea), (count_hbm, count)))]
        large = [pltpu.make_async_copy(state_hbm.at[pl.ds(2 * f, 2)], state.at[pl.ds(2 * f, 2)], in_sem.at[3 + f])
                 for f in range(2)]
        for copy in small + large:
            copy.start()

        flip = 1 - core
        y_east, y_west = y + core, y + ny - flip
        place = {
            1: (lax.rem(x + lax.div(y_east, ny), nx), lax.rem(y_east, ny), flip),
            -1: (lax.rem(x + nx - 1 + lax.div(y_west, ny), nx), lax.rem(y_west, ny), flip),
            0: (x, y, core),
        }
        row = {1: lax.rem(lat + 1, nlat), -1: lax.rem(lat + nlat - 1, nlat), 0: lat}
        near = [(*place[dx], row[dy]) for dx, dy in DIRS]

        def hops(step, size):
            return min(step, size - step)

        plane_steps = sorted(((i, j) for i in range(nx) for j in range(ny) if i or j),
                             key=lambda p: -hops(p[0], nx) - hops(p[1], ny))
        xs = [x] + [lax.rem(x + i, nx) for i in range(1, nx)]
        ys = [y] + [lax.rem(y + j, ny) for j in range(1, ny)]
        plane_peer = [(xs[i], ys[j], core, lat) for i, j in plane_steps]
        line_steps = sorted(((c, j) for c in range(CORES) for j in range(nlat) if c or j),
                            key=lambda p: -hops(p[1], nlat))
        lats = [lat] + [lax.rem(lat + j, nlat) for j in range(1, nlat)]
        line_peer = [(x, y, (core, flip)[c], lats[j]) for c, j in line_steps]
        barrier = pltpu.get_barrier_semaphore()
        column = [(x, p, core, lat) for p in ys[1:]]
        rows = [(p, y, core, lat) for p in xs[1:]]
        along = [(x, y, c, lax.rem(lat + j, nlat)) for j in (2, nlat - 2, 1, nlat - 1) for c in (core, flip)]
        relay = column + [(x, y, core, lax.rem(lat + j, nlat)) for j in (2, nlat - 2)]
        peers = [near[NW], near[W]] + along[:4] + column + rows + along[4:] + [near[N], (x, y, flip, lat)]
        for peer in peers:
            pl.semaphore_signal(barrier, inc=1, device_id=peer, device_id_type=MESH)

        lane = iota((8, 128), 1)
        sub = iota((8, 128), 0)

        for copy in small:
            copy.wait()
        wet = sea[...] * count[...]
        for t in range(3):
            rows = slice(8 * t, 8 * t + 8)
            surf[t, 0] = wet[rows].astype(F32)
            surf[t, 1] = (sea[rows].astype(F32) * forcing[rows]) * 65536.0

        partial[...] = jnp.zeros_like(partial)
        mid[...] = jnp.zeros_like(mid)
        pl.semaphore_wait(barrier, len(peers))

        def remote(source, target, i, peer):
            return pltpu.make_async_remote_copy(source, target, send_sem.at[i], recv_sem.at[i],
                                                device_id=peer, device_id_type=MESH)

        def surf_copy(d, tiles, target, group):
            return remote(surf.at[pl.ds(*tiles)], target, group, near[d])

        def rows_copy(d, part):
            source = rows_up if DIRS[d][1] > 0 else rows_down
            span = pl.ds(0, half) if part == 0 else pl.ds(half, entries - half)
            return remote(source.at[span], (rows_a, rows_b)[part].at[OPP[d] - 2], 1 + part, near[d])

        def corner_copy(d):
            source = rows_up if DIRS[d][1] > 0 else rows_down
            return remote(source.at[pl.ds(levels, groups)], corners_in.at[OPP[d] - 4], 3, near[d])

        def edge_copy(d):
            return remote(edges, edges_in.at[OPP[d]], 4, near[d])

        landing = (surf_in, rows_a, rows_b, corners_in, edges_in, gather_a, gather_b, surf_s, surf_b)

        def wait_all(sem, i):
            pltpu.make_async_copy(landing[i], landing[i], sem.at[i]).wait()

        surf_copy(SE, (0, 2), surf_in.at[pl.ds(5, 2)], 0).start()
        surf_copy(E, (0, 3), surf_in.at[pl.ds(0, 3)], 0).start()
        surf_copy(S, (0, 2), surf_in.at[pl.ds(3, 2)], 0).start()
        surf_copy(N, (2, 1), surf_s, 7).start()
        for peer in relay:
            pl.semaphore_signal(ready, inc=1, device_id=peer, device_id_type=MESH)
        for copy in large:
            copy.wait()

        lane24 = iota((24, 128), 1)

        def pack_edges(f, carry):
            for g in range(groups):
                packed = jnp.zeros((24, 128), F32)
                for i in range(min(GROUP, levels - g * GROUP)):
                    moved = pltpu.roll(state[f, g * GROUP + i], (4 + 8 * i) % 128, 1)
                    packed = jnp.where(lane24 // 8 == i, moved, packed)
                edges[f, g] = packed
            return carry


        def packed_rows(tile_of):
            up, down = None, None
            for f in range(4):
                top = pltpu.roll(tile_of(f, slice(16, 24)), (2 * f + 2) % 8, 0)
                low = tile_of(f, slice(0, 8))
                low = pltpu.roll(low, 2 * f, 0) if f else low
                up = top if f == 0 else jnp.where(sub // 2 == f, top, up)
                down = low if f == 0 else jnp.where(sub // 2 == f, low, down)
            return up, down

        def pack_rows(k, carry):
            up, down = packed_rows(lambda f, rows: state[f, k, rows])
            rows_up[k] = up
            rows_down[k] = down
            return carry

        lax.fori_loop(0, levels, pack_rows, 0)
        for d in (N, S):
            rows_copy(d, 0).start()
        lax.fori_loop(0, 4, pack_edges, 0)
        for g in range(groups):
            up, down = packed_rows(lambda f, rows: edges[f, g, rows])
            rows_up[levels + g] = up
            rows_down[levels + g] = down

        for d in (N, S):
            rows_copy(d, 1).start()
        wait_all(recv_sem, 0)

        has_north = jnp.where(lat < nlat - 1, 1.0, 0.0).astype(F32)
        has_south = jnp.where(lat > 0, 1.0, 0.0).astype(F32)

        def ahead(v):
            own = [surf[t, v] for t in range(3)] + [surf_in[3 + t, v] for t in range(2)]
            west = [surf_in[t, v] for t in range(3)] + [surf_in[5 + t, v] for t in range(2)]
            return jnp.concatenate(own, 0), jnp.concatenate(west, 0)

        def around_own(v):
            own = [surf[t, v] for t in range(3)] + [surf_in[3, v] * has_north, surf_s[0, v] * has_south]
            side = [jnp.where(lane < 64, surf_b[t, v], surf_in[t, v]) for t in range(3)]
            side.append(jnp.where(lane < 64, surf_b[3, v], surf_in[5, v]) * has_north)
            side.append(jnp.where(lane < 64, surf_b[4, v], surf_b[5, v]) * has_south)
            return jnp.concatenate(own, 0), jnp.concatenate(side, 0)

        lane40 = iota((40, 128), 1)

        def to_east(pair):
            a, b = shift_lanes(pair[0], 1), shift_lanes(pair[1], 1)
            return jnp.where(lane40 == 127, b, a), jnp.where(lane40 == 127, a, b)

        def to_west(pair):
            a, b = shift_lanes(pair[0], -1), shift_lanes(pair[1], -1)
            return jnp.where(lane40 == 0, b, a), jnp.where(lane40 == 0, a, b)

        def to_north(pair):
            return shift_rows(pair[0], 1), shift_rows(pair[1], 1)

        def to_south(pair):
            return shift_rows(pair[0], -1), shift_rows(pair[1], -1)

        moves = (to_east, to_west, to_north, to_south)
        def krylov(depth, force, both, cuts=None):
            moved = [move(depth) for move in moves]
            faces = [[jnp.minimum(depth[t], m[t]) for m in moved] for t in range(2)]
            if cuts is not None:
                faces = [[e, w, n * cuts[0], s * cuts[1]] for e, w, n, s in faces]
            diag = [2.0 + ((faces[t][0] + faces[t][1]) + (faces[t][2] + faces[t][3])) for t in range(2)]
            inverse = [1.0 / diag[t] for t in range(2)]

            def over_diag(hi, lo, t):
                q, _ = short(hi * inverse[t], 0.0)
                return q, ((hi - diag[t] * q) + lo) * inverse[t]

            vectors = [[short(*over_diag(force[t], 0.0, t)) for t in range(2)]]
            for k in range(4):
                last = vectors[-1]
                high = [move((last[0][0], last[1][0])) for move in moves]
                low = [move((last[0][1], last[1][1])) for move in moves]
                following = []
                for t in range(2 if both or k < 3 else 1):
                    terms = [faces[t][i] * high[i][t] for i in range(4)]
                    fine = [faces[t][i] * low[i][t] for i in range(4)]
                    s0, e0 = two_sum(terms[0], terms[1])
                    s1, e1 = two_sum(terms[2], terms[3])
                    s, e2 = two_sum(s0, s1)
                    rest = ((e0 + e1) + e2) + ((fine[0] + fine[1]) + (fine[2] + fine[3]))
                    q, q_low = over_diag(s, rest, t)
                    s, e = two_sum(last[t][0], -q)
                    following.append(short(s, e + (last[t][1] - q_low)))
                vectors.append(following)
            return diag, vectors

        def counted(pair):
            cells = jnp.where(lane40 < 128 - HALO, pair[0], pair[1])
            first = jnp.where(sub < HALO, cells[24:32], cells[0:8])
            return jnp.concatenate([first, cells[8:24]], 0)

        row40 = iota((40, 128), 0)
        cuts = [jnp.where(row40 == row, has_north, 1.0) for row in (23, 24)]
        diag, vectors = krylov(ahead(0), ahead(1), True, cuts)
        terms = [tuple(counted((v[0][i], v[1][i])) for i in range(2)) for v in vectors]
        scale = counted(diag)
        weighted = [quick(scale * hi, scale * lo) for hi, lo in terms[:4]]
        terms = [quick(hi, lo) for hi, lo in terms]

        sums = []
        for n in range(8):
            product = dd_mul(weighted[n // 2], terms[n - n // 2])
            tiles = [(product[0][8 * i:8 * i + 8], product[1][8 * i:8 * i + 8]) for i in range(3)]
            sums.append(dd_add(dd_add(tiles[0], tiles[1]), tiles[2]))

        def fold(a, b, near_mask, step):
            def one(i):
                x, y = a[i], b[i]
                far = jnp.where(near_mask, pltpu.roll(x, 8 - step, 0), pltpu.roll(y, step, 0))
                return jnp.where(near_mask, x, y), far
            kept, far = zip(*(one(i) for i in range(2)))
            return dd_add(kept, far)

        level = [fold(sums[2 * i], sums[2 * i + 1], sub < 4, 4) for i in range(4)]
        level = [fold(level[2 * i], level[2 * i + 1], sub % 4 < 2, 2) for i in range(2)]
        level = fold(level[0], level[1], sub % 2 < 1, 1)
        parts = [x.T for x in level]
        parts = [tuple(p[8 * i:8 * i + 8] for p in parts) for i in range(16)]
        while len(parts) > 1:
            parts = [dd_add(parts[i], parts[i + 1]) for i in range(0, len(parts), 2)]
        level = parts[0]
        for step in (4, 2, 1):
            level = dd_add(tuple(p[:step] for p in level), tuple(p[step:2 * step] for p in level))
        partial[0:1, 0:8] = level[0]
        partial[1:2, 0:8] = level[1]

        pl.semaphore_wait(ready, len(relay))
        for j, peer in enumerate(plane_peer):
            remote(partial, gather_a.at[j], 5, peer).start()
        surf_copy(NE, (2, 1), surf_b.at[pl.ds(5, 1)], 8).start()
        surf_copy(NW, (2, 1), surf_b.at[pl.ds(4, 1)], 8).start()
        surf_copy(SW, (0, 1), surf_b.at[pl.ds(3, 1)], 8).start()
        surf_copy(W, (0, 3), surf_b.at[pl.ds(0, 3)], 8).start()
        for d in (NE, NW, SE, SW):
            corner_copy(d).start()
        for d in (E, W):
            edge_copy(d).start()

        def total(own, others, number):
            parts = [(own[0:1], own[1:2])] + [(others[j, 0:1], others[j, 1:2]) for j in range(number)]
            while len(parts) > 1:
                parts = [dd_add(parts[i], parts[i + 1]) if i + 1 < len(parts) else parts[i]
                         for i in range(0, len(parts), 2)]
            return parts[0]

        wait_all(recv_sem, 1)
        wait_all(recv_sem, 7)
        south_count, north_count = surf_s[0, 0] * has_south, surf_in[3, 0] * has_north
        count_own = jnp.concatenate([surf[t, 0] for t in range(3)] + [jnp.where(sub < 4, north_count, south_count)], 0)

        def with_rows(f, block, north, south):
            up = pltpu.roll(north, (8 - 2 * f) % 8, 0) if f else north
            down = pltpu.roll(south, 6 - 2 * f, 0) if f < 3 else south
            return jnp.concatenate([block, jnp.where(sub < 4, up, down)], 0)

        def main(k, slot, rows_in, base):
            active = jnp.where(count_own > k.astype(F32), 1.0, 0.0)
            north, south = rows_in[N - 2, k - base], rows_in[S - 2, k - base]
            quads = [with_rows(f, state[f, k], north, south) for f in range(4)]
            for f, value in enumerate(first_pass(active, quads, masked.at[slot], laps.at[k - base], weight.at[k - base])):
                tend[f, k] = value

        def finish(k, base):
            for f in range(4):
                tend[f, k] = tend[f, k] - second_pass(f, laps.at[k - base], weight.at[k - base])

        def unrolled(body, first, last, by):
            def step(i, carry):
                for j in range(by):
                    body(first + i * by + j, j)
                return carry
            lax.fori_loop(0, (last - first) // by, step, 0)

        unrolled(lambda k, slot: main(k, slot, rows_a, 0), 0, half, UNROLL)
        unrolled(lambda k, slot: finish(k, 0), 0, half, FINISH)

        wait_all(recv_sem, 5)
        hi, lo = total(partial, gather_a, nplane - 1)
        mid[0:1] = hi
        mid[1:2] = lo
        for j, peer in enumerate(line_peer):
            remote(mid, gather_b.at[j], 6, peer).start()

        wait_all(recv_sem, 2)
        unrolled(lambda k, slot: main(k, slot, rows_b, half), half, levels, UNROLL)
        unrolled(lambda k, slot: finish(k, half), half, levels, FINISH)
        wait_all(recv_sem, 8)
        depth = around_own(0)
        diag, vectors = krylov(depth, around_own(1), False)
        own_vectors = [quick(v[0][0][:24], v[0][1][:24]) for v in vectors]
        own_diag = diag[0][:24]
        count_side = jnp.concatenate([depth[1][:24], jnp.where(sub < 4, depth[1][24:32], depth[1][32:40])], 0)
        lane32 = iota((32, 128), 1)

        def spread(first, second):
            x = jnp.where(lane32 < 8, jnp.where(lane32 < 4, pltpu.roll(first, 4, 1), pltpu.roll(second, 4, 1)), 0.0)
            for step in (8, 16, 32, 64):
                x = x + pltpu.roll(x, step, 1)
            return x

        counts[0] = spread(count_side, count_own)
        counts[1] = spread(count_own, count_side)

        wait_all(recv_sem, 3)
        wait_all(recv_sem, 4)
        left24, left8 = lane24 % 8 < 4, lane % 8 < 4

        def edge_active(side, g):
            return jnp.where(counts[side] > (lane32 // 8 + g * GROUP).astype(F32), 1.0, 0.0)

        def edge_first(g, side, slot):
            if side == 0:
                north = jnp.where(left8, corners_in[NW - 4, g], rows_b[N - 2, levels - half + g])
                south = jnp.where(left8, corners_in[SW - 4, g], rows_b[S - 2, levels - half + g])
                blocks = [jnp.where(left24, edges_in[W, f, g], edges[f, g]) for f in range(4)]
            else:
                north = jnp.where(left8, rows_b[N - 2, levels - half + g], corners_in[NE - 4, g])
                south = jnp.where(left8, rows_b[S - 2, levels - half + g], corners_in[SE - 4, g])
                blocks = [jnp.where(left24, edges[f, g], edges_in[E, f, g]) for f in range(4)]
            quads = [with_rows(f, blocks[f], north, south) for f in range(4)]
            at = 2 * g + side
            return first_pass(edge_active(side, g), quads, masked.at[slot], laps.at[at], weight.at[at])

        def edge(g):
            west, east = edge_first(g, 0, 0), edge_first(g, 1, 1)
            for f in range(4):
                edge_out[f, g] = jnp.where(left24, east[f], west[f])

        def edge_finish(g):
            for f in range(4):
                west, east = (second_pass(f, laps.at[2 * g + i], weight.at[2 * g + i]) for i in range(2))
                edge_out[f, g] = edge_out[f, g] - jnp.where(left24, east, west)

        unrolled(lambda g, slot: edge(g), 0, groups, 1)
        unrolled(lambda g, slot: edge_finish(g), 0, groups, groups)

        rim = (lane24 < 2) | (lane24 >= 126)

        for k in range(levels):
            g, back = k // GROUP, (252 - 8 * (k % GROUP)) % 128
            for f in range(4):
                tend[f, k] = jnp.where(rim, pltpu.roll(edge_out[f, g], back, 1), tend[f, k])

        wait_all(recv_sem, 6)
        level = total(mid, gather_b, nline - 1)

        def scalar(a, n):
            return jnp.broadcast_to(a[0:1, n:n + 1], (8, 128))

        mu = []
        for n in range(8):
            at = 4 * (n % 2) + 2 * (n // 2 % 2) + n // 4
            mu.append((scalar(level[0], at), scalar(level[1], at)))
        x_poly, r_poly = cg_coefficients(mu)
        for t in range(3):
            rows = slice(8 * t, 8 * t + 8)
            basis = [(v[0][rows], v[1][rows]) for v in own_vectors]

            def combined(poly):
                parts = [dd_mul(c, b) for c, b in zip(poly, basis)]
                while len(parts) > 1:
                    parts = [dd_add(parts[i], parts[i + 1]) if i + 1 < len(parts) else parts[i]
                             for i in range(0, len(parts), 2)]
                return parts[0]

            height = combined(x_poly)
            x_ref[rows] = (height[0] + height[1]) * (40.0 / 65536.0)
            rest = combined(r_poly)
            d = own_diag[rows]
            r_ref[rows] = (d * rest[0] + d * rest[1]) * (1.0 / 65536.0)

        for i in range(9):
            wait_all(send_sem, i)

    scratch = [
        pltpu.VMEM((24, 128), F32), pltpu.VMEM((24, 128), jnp.int32), pltpu.VMEM((24, 128), jnp.int32),
        pltpu.VMEM((4, levels, 24, 128), F32),
        pltpu.VMEM((3, 2, 8, 128), F32), pltpu.VMEM((7, 2, 8, 128), F32),
        pltpu.VMEM((1, 2, 8, 128), F32), pltpu.VMEM((6, 2, 8, 128), F32),
        pltpu.VMEM((4, groups, 24, 128), F32), pltpu.VMEM((2, 4, groups, 24, 128), F32),
        pltpu.VMEM((entries, 8, 128), F32), pltpu.VMEM((entries, 8, 128), F32),
        pltpu.VMEM((2, half, 8, 128), F32), pltpu.VMEM((2, entries - half, 8, 128), F32),
        pltpu.VMEM((4, groups, 8, 128), F32),
        pltpu.VMEM((2, 32, 128), F32), pltpu.VMEM((UNROLL, 4, 48, 128), F32),
        pltpu.VMEM((half, 4, 40, 128), F32), pltpu.VMEM((half, 24, 128), F32),
        pltpu.VMEM((4, groups, 24, 128), F32),
        pltpu.VMEM((2, 128), F32), pltpu.VMEM((nplane - 1, 2, 128), F32),
        pltpu.VMEM((2, 128), F32), pltpu.VMEM((nline - 1, 2, 128), F32),
        pltpu.SemaphoreType.DMA((5,)), pltpu.SemaphoreType.DMA((9,)), pltpu.SemaphoreType.DMA((9,)),
        pltpu.SemaphoreType.REGULAR,
    ]
    return kernel, scratch


def hand_out(x_ref, r_ref, tend_ref, x_out, r_out, tend_out, sem):
    copies = [pltpu.make_async_copy(tend_ref.at[f], tend_out.at[f], sem.at[f]) for f in range(4)]
    copies += [pltpu.make_async_copy(x_ref, x_out, sem.at[4]), pltpu.make_async_copy(r_ref, r_out, sem.at[5])]
    for copy in copies:
        copy.start()
    for copy in copies:
        copy.wait()


def solution(mesh):
    nlon, nlat = mesh.shape["lon"], mesh.shape["lat"]
    nplane = nlon // CORES
    nx = max(n for n in range(1, nplane + 1) if nplane % n == 0 and n * n <= nplane)
    ny = nplane // nx
    finer = Mesh(mesh.devices.reshape(nx, ny, CORES, nlat), ("x", "y", "core", "lat"))

    def per_device(surface_forcing, sea_mask, level_count, state):
        kernel, scratch = make_kernel(nx, ny, nlat, state.shape[1])
        results = pl.pallas_call(
            kernel,
            out_shape=(
                pltpu.VMEM(surface_forcing.shape, F32),
                pltpu.VMEM(surface_forcing.shape, F32),
                pltpu.VMEM(state.shape, F32),
            ),
            in_specs=[pl.BlockSpec(memory_space=pl.ANY)] * 4,
            out_specs=(
                pl.BlockSpec(memory_space=pltpu.VMEM),
                pl.BlockSpec(memory_space=pltpu.VMEM),
                pl.BlockSpec(memory_space=pltpu.VMEM),
            ),
            scratch_shapes=scratch,
            compiler_params=pltpu.CompilerParams(collective_id=0, has_side_effects=True, vmem_limit_bytes=65_030_000),
            name="ocean",
        )(surface_forcing, sea_mask, level_count, state)
        return pl.pallas_call(
            hand_out,
            out_shape=tuple(jax.ShapeDtypeStruct(r.shape, F32) for r in results),
            in_specs=[pl.BlockSpec(memory_space=pltpu.VMEM)] * 3,
            out_specs=[pl.BlockSpec(memory_space=pl.ANY)] * 3,
            scratch_shapes=[pltpu.SemaphoreType.DMA((6,))],
            compiler_params=pltpu.CompilerParams(vmem_limit_bytes=8 * 2**20),
            name="hand_out",
        )(*results)

    flat, deep = P("lat", ("x", "y", "core")), P(None, None, "lat", ("x", "y", "core"))
    return jax.shard_map(
        per_device, mesh=finer, in_specs=(flat, flat, flat, deep), out_specs=(flat, flat, deep), check_vma=False
    )
```

```python
import jax
import jax.numpy as jnp
from jax import lax
from jax.experimental import pallas as pl
from jax.experimental.pallas import tpu as pltpu
from jax.sharding import Mesh
from jax.sharding import PartitionSpec as P

MESH = pl.DeviceIdType.MESH
F32 = jnp.float32
CORES = 2
GROUP = 16
VISC = 0.02
HALO = 5
UNROLL = 2
FINISH = 4
DIRS = ((1, 0), (-1, 0), (0, 1), (0, -1), (1, 1), (-1, -1), (1, -1), (-1, 1))
OPP = (1, 0, 3, 2, 5, 4, 7, 6)
E, W, N, S, NE, SW, SE, NW = range(8)


def two_sum(a, b):
    s = a + b
    t = s - a
    return s, (a - (s - t)) + (b - t)


def quick(a, b):
    s = a + b
    return s, b - (s - a)


def split(a):
    t = 4097.0 * a
    h = t - (t - a)
    return h, a - h


def two_prod(a, b):
    p = a * b
    ah, al = split(a)
    bh, bl = split(b)
    return p, ((ah * bh - p) + ah * bl + al * bh) + al * bl


def short(hi, lo):
    t = 257.0 * hi
    h = t - (t - hi)
    return h, (hi - h) + lo


def dd_add(a, b):
    s, e = two_sum(a[0], b[0])
    return quick(s, e + (a[1] + b[1]))


def dd_mul(a, b):
    p, e = two_prod(a[0], b[0])
    return p, e + (a[0] * b[1] + a[1] * b[0])


def dd_neg(a):
    return -a[0], -a[1]


def dd_div(a, b, r):
    q = a[0] * r
    p, e = two_prod(q, b[0])
    rest = ((a[0] - p) - e) + (a[1] - q * b[1])
    return q, rest * r


def iota(shape, dim):
    return lax.broadcasted_iota(jnp.int32, shape, dim)


def shift_rows(x, step):
    return pltpu.roll(x, (-step) % x.shape[0], 0)


def shift_lanes(x, step):
    return pltpu.roll(x, (-step) % 128, 1)


def cg_coefficients(mu):
    s, t = dict(enumerate(mu)), dict(enumerate(mu))
    one = (jnp.ones_like(mu[0][0]), jnp.zeros_like(mu[0][0]))
    p, q = [one], [one]
    x = []
    for k in range(4):
        inverse = 1.0 / t[k + 1][0]
        alpha = dd_div(s[k], t[k + 1], inverse)
        minus = dd_neg(alpha)
        x = [dd_add(x[i], dd_mul(alpha, q[i])) if i < len(x) else dd_mul(alpha, q[i]) for i in range(k + 1)]
        moved = [dd_mul(minus, c) for c in q]
        p = [p[i] if i == 0 else (dd_add(p[i], moved[i - 1]) if i <= k else moved[i - 1]) for i in range(k + 2)]
        if k < 3:
            last = 6 - k
            s_next = {j: dd_add(s[j], dd_mul(minus, t[j + 1])) for j in range(k + 1, last + 1)}
            beta = dd_div(dd_neg(s_next[k + 1]), t[k + 1], inverse)
            t = {j: dd_add(s_next[j], dd_mul(beta, t[j])) for j in range(k + 2, last + 1)}
            s = s_next
            q = [dd_add(p[i], dd_mul(beta, q[i])) if i <= k else p[i] for i in range(k + 2)]
    return x, p


def first_pass(active, quads, masked, laps, weight):
    own = slice(0, 24)
    face_e, face_w = active * shift_lanes(active, 1), active * shift_lanes(active, -1)
    face_n, face_s = active * shift_rows(active, 1), active * shift_rows(active, -1)
    count = (face_e + face_w) + (face_n + face_s)
    weight[...] = VISC * active[own]
    visc_count = VISC * count[own]
    near = []
    for f, q in enumerate(quads):
        q = active * q
        masked[f, 0:8] = q[24:32]
        masked[f, 8:40] = q
        masked[f, 40:48] = q[0:8]
        near.append((q, shift_lanes(q, 1), shift_lanes(q, -1)))
    u, ue, uw = (x[own] for x in near[2])
    v = near[3][0][own]
    flow_e = (0.25 * face_e[own]) * (u + ue)
    flow_w = (0.25 * face_w[own]) * (u + uw)
    flow_n = (0.25 * face_n[own]) * (v + masked[3, 9:33])
    flow_s = (0.25 * face_s[own]) * (v + masked[3, 7:31])
    net = (flow_e - flow_w) + (flow_n - flow_s)
    out = []
    for f, (q, qe, qw) in enumerate(near):
        qn, qs = masked[f, 9:41], masked[f, 7:39]
        lap = active * ((qe + qw) + (qn + qs)) - count * q
        laps[f, 0:8] = lap[24:32]
        laps[f, 8:40] = lap
        flux = (net * q[own] + flow_e * qe[own]) + (flow_n * qn[own] - flow_w * qw[own]) - flow_s * qs[own]
        out.append(visc_count * lap[own] - flux)
    return out


def second_pass(f, laps, weight):
    lap = laps[f, 8:32]
    around = (shift_lanes(lap, 1) + shift_lanes(lap, -1)) + (laps[f, 9:33] + laps[f, 7:31])
    return weight[...] * around


def make_kernel(nx, ny, nlat, levels):
    nplane = nx * ny
    nline = CORES * nlat
    half = 7 * levels // 10
    groups = -(-levels // GROUP)
    entries = levels + groups
    def kernel(forcing_hbm, sea_hbm, count_hbm, state_hbm, x_ref, r_ref, tend,
               forcing, sea, count, state, surf, surf_in, surf_s, surf_b, surf_n, edges, edges_in, rows_up, rows_down,
               rows_a, rows_b, corners_in, counts, masked, laps, weight, edge_out, partial, gather_a, mid, gather_b, in_sem, send_sem, recv_sem, ready):
        x, y = lax.axis_index("x"), lax.axis_index("y")
        core, lat = lax.axis_index("core"), lax.axis_index("lat")

        small = [pltpu.make_async_copy(a, b, in_sem.at[i]) for i, (a, b) in
                 enumerate(((forcing_hbm, forcing), (sea_hbm, sea), (count_hbm, count)))]
        large = [pltpu.make_async_copy(state_hbm.at[pl.ds(2 * f, 2)], state.at[pl.ds(2 * f, 2)], in_sem.at[3 + f])
                 for f in range(2)]
        for copy in small + large:
            copy.start()

        flip = 1 - core
        y_east, y_west = y + core, y + ny - flip
        place = {
            1: (lax.rem(x + lax.div(y_east, ny), nx), lax.rem(y_east, ny), flip),
            -1: (lax.rem(x + nx - 1 + lax.div(y_west, ny), nx), lax.rem(y_west, ny), flip),
            0: (x, y, core),
        }
        row = {1: lax.rem(lat + 1, nlat), -1: lax.rem(lat + nlat - 1, nlat), 0: lat}
        near = [(*place[dx], row[dy]) for dx, dy in DIRS]

        def hops(step, size):
            return min(step, size - step)

        plane_steps = sorted(((i, j) for i in range(nx) for j in range(ny) if i or j),
                             key=lambda p: -hops(p[0], nx) - hops(p[1], ny))
        xs = [x] + [lax.rem(x + i, nx) for i in range(1, nx)]
        ys = [y] + [lax.rem(y + j, ny) for j in range(1, ny)]
        plane_peer = [(xs[i], ys[j], core, lat) for i, j in plane_steps]
        line_steps = sorted(((c, j) for c in range(CORES) for j in range(nlat) if c or j),
                            key=lambda p: -hops(p[1], nlat))
        lats = [lat] + [lax.rem(lat + j, nlat) for j in range(1, nlat)]
        line_peer = [(x, y, (core, flip)[c], lats[j]) for c, j in line_steps]
        barrier = pltpu.get_barrier_semaphore()
        column = [(x, p, core, lat) for p in ys[1:]]
        rows = [(p, y, core, lat) for p in xs[1:]]
        along = [(x, y, c, lax.rem(lat + j, nlat)) for j in (2, nlat - 2, 1, nlat - 1) for c in (core, flip)]
        relay = column + [(x, y, core, lax.rem(lat + j, nlat)) for j in (2, nlat - 2)]
        peers = [near[NW], near[W]] + along[:4] + column + rows + along[4:] + [near[N], (x, y, flip, lat)]
        for peer in peers:
            pl.semaphore_signal(barrier, inc=1, device_id=peer, device_id_type=MESH)

        lane = iota((8, 128), 1)
        sub = iota((8, 128), 0)

        for copy in small:
            copy.wait()
        wet = sea[...] * count[...]
        for t in range(3):
            rows = slice(8 * t, 8 * t + 8)
            surf[t, 0] = wet[rows].astype(F32)
            surf[t, 1] = (sea[rows].astype(F32) * forcing[rows]) * 65536.0

        partial[...] = jnp.zeros_like(partial)
        mid[...] = jnp.zeros_like(mid)
        pl.semaphore_wait(barrier, len(peers))

        def remote(source, target, i, peer):
            return pltpu.make_async_remote_copy(source, target, send_sem.at[i], recv_sem.at[i],
                                                device_id=peer, device_id_type=MESH)

        def surf_copy(d, tiles, target, group):
            return remote(surf.at[pl.ds(*tiles)], target, group, near[d])

        def rows_copy(d, part):
            source = rows_up if DIRS[d][1] > 0 else rows_down
            span = pl.ds(0, half) if part == 0 else pl.ds(half, entries - half)
            return remote(source.at[span], (rows_a, rows_b)[part].at[OPP[d] - 2], 1 + part, near[d])

        def corner_copy(d):
            source = rows_up if DIRS[d][1] > 0 else rows_down
            return remote(source.at[pl.ds(levels, groups)], corners_in.at[OPP[d] - 4], 3, near[d])

        def edge_copy(d):
            return remote(edges, edges_in.at[OPP[d]], 4, near[d])

        landing = (surf_in, rows_a, rows_b, corners_in, edges_in, gather_a, gather_b, surf_s, surf_b, surf_n)

        def wait_all(sem, i):
            pltpu.make_async_copy(landing[i], landing[i], sem.at[i]).wait()

        southward = (surf_copy(SE, (0, 2), surf_n.at[pl.ds(2, 2)], 9), surf_copy(S, (0, 2), surf_n.at[pl.ds(0, 2)], 9))

        @pl.when(lat > 0)
        def _():
            southward[0].start()

        surf_copy(E, (0, 3), surf_in, 0).start()

        @pl.when(lat > 0)
        def _():
            southward[1].start()

        surf_copy(N, (2, 1), surf_s, 7).start()
        for peer in relay:
            pl.semaphore_signal(ready, inc=1, device_id=peer, device_id_type=MESH)
        for copy in large:
            copy.wait()

        lane24 = iota((24, 128), 1)

        def pack_edges(f, carry):
            for g in range(groups):
                packed = jnp.zeros((24, 128), F32)
                for i in range(min(GROUP, levels - g * GROUP)):
                    moved = pltpu.roll(state[f, g * GROUP + i], (4 + 8 * i) % 128, 1)
                    packed = jnp.where(lane24 // 8 == i, moved, packed)
                edges[f, g] = packed
            return carry


        def packed_rows(tile_of):
            up, down = None, None
            for f in range(4):
                top = pltpu.roll(tile_of(f, slice(16, 24)), (2 * f + 2) % 8, 0)
                low = tile_of(f, slice(0, 8))
                low = pltpu.roll(low, 2 * f, 0) if f else low
                up = top if f == 0 else jnp.where(sub // 2 == f, top, up)
                down = low if f == 0 else jnp.where(sub // 2 == f, low, down)
            return up, down

        def pack_rows(k, carry):
            up, down = packed_rows(lambda f, rows: state[f, k, rows])
            rows_up[k] = up
            rows_down[k] = down
            return carry

        lax.fori_loop(0, levels, pack_rows, 0)
        for d in (N, S):
            rows_copy(d, 0).start()
        lax.fori_loop(0, 4, pack_edges, 0)
        for g in range(groups):
            up, down = packed_rows(lambda f, rows: edges[f, g, rows])
            rows_up[levels + g] = up
            rows_down[levels + g] = down

        wait_all(recv_sem, 0)

        @pl.when(lat < nlat - 1)
        def _():
            wait_all(recv_sem, 9)


        has_south = jnp.where(lat > 0, 1.0, 0.0).astype(F32)

        def from_north(tile, v):
            return jnp.where(lat < nlat - 1, surf_n[tile, v], 0.0)

        def ahead(v):
            own = [surf[t, v] for t in range(3)] + [from_north(t, v) for t in range(2)]
            west = [surf_in[t, v] for t in range(3)] + [from_north(2 + t, v) for t in range(2)]
            return jnp.concatenate(own, 0), jnp.concatenate(west, 0)

        def around_own(v):
            own = [surf[t, v] for t in range(3)] + [from_north(0, v), surf_s[0, v] * has_south]
            side = [jnp.where(lane < 64, surf_b[t, v], surf_in[t, v]) for t in range(3)]
            side.append(jnp.where(lane < 64, jnp.where(lat < nlat - 1, surf_b[3, v], 0.0), from_north(2, v)))
            side.append(jnp.where(lane < 64, surf_b[4, v], surf_b[5, v]) * has_south)
            return jnp.concatenate(own, 0), jnp.concatenate(side, 0)

        lane40 = iota((40, 128), 1)

        def to_east(pair):
            a, b = shift_lanes(pair[0], 1), shift_lanes(pair[1], 1)
            last = iota(a.shape, 1) == 127
            return jnp.where(last, b, a), jnp.where(last, a, b)

        def to_west(pair):
            a, b = shift_lanes(pair[0], -1), shift_lanes(pair[1], -1)
            first = iota(a.shape, 1) == 0
            return jnp.where(first, b, a), jnp.where(first, a, b)

        def to_north(pair):
            return shift_rows(pair[0], 1), shift_rows(pair[1], 1)

        def to_south(pair):
            return shift_rows(pair[0], -1), shift_rows(pair[1], -1)

        moves = (to_east, to_west, to_north, to_south)
        def krylov(depth, force, both, cut=None, kept=40):
            moved = [move(depth) for move in moves]
            faces = [[jnp.minimum(depth[t], m[t]) for m in moved] for t in range(2)]
            if cut is not None:
                faces = [[e, w, n, s * cut] for e, w, n, s in faces]
            diag = [2.0 + ((faces[t][0] + faces[t][1]) + (faces[t][2] + faces[t][3])) for t in range(2)]
            inverse = [1.0 / diag[t] for t in range(2)]

            def over_diag(hi, lo, t):
                q, _ = short(hi * inverse[t], 0.0)
                return q, ((hi - diag[t] * q) + lo) * inverse[t]

            vectors = [[short(*over_diag(force[t], 0.0, t)) for t in range(2)]]
            for k in range(4):
                last = vectors[-1]
                high = [move((last[0][0], last[1][0])) for move in moves]
                low = [move((last[0][1], last[1][1])) for move in moves]
                if k == 0 and kept < 40:
                    high, low = ([[x[:kept] for x in pair] for pair in part] for part in (high, low))
                    last = [tuple(x[:kept] for x in pair) for pair in last]
                    faces = [[x[:kept] for x in part] for part in faces]
                    diag, inverse = [x[:kept] for x in diag], [x[:kept] for x in inverse]
                following = []
                for t in range(2 if both or k < 3 else 1):
                    terms = [faces[t][i] * high[i][t] for i in range(4)]
                    fine = [faces[t][i] * low[i][t] for i in range(4)]
                    s0, e0 = two_sum(terms[0], terms[1])
                    s1, e1 = two_sum(terms[2], terms[3])
                    s, e2 = two_sum(s0, s1)
                    rest = ((e0 + e1) + e2) + ((fine[0] + fine[1]) + (fine[2] + fine[3]))
                    q, q_low = over_diag(s, rest, t)
                    s, e = two_sum(last[t][0], -q)
                    following.append(short(s, e + (last[t][1] - q_low)))
                vectors.append(following)
            return diag, vectors

        def counted(pair):
            cells = jnp.where(iota(pair[0].shape, 1) < 128 - HALO, pair[0], pair[1])
            first = jnp.where(sub < HALO, cells[24:32], cells[0:8])
            return jnp.concatenate([first, cells[8:24], jnp.where(sub < southern, cells[0:8], 0.0)], 0)

        southern = jnp.where(lat > 0, 0, HALO)
        cut = jnp.where(iota((40, 128), 0) == 0, has_south, 1.0)
        diag, vectors = krylov(ahead(0), ahead(1), True, cut, 32)
        terms = [tuple(counted((v[0][i], v[1][i])) for i in range(2)) for v in vectors]
        scale = counted(diag)
        weighted = [quick(scale * hi, scale * lo) for hi, lo in terms[:4]]
        terms = [quick(hi, lo) for hi, lo in terms]

        sums = []
        for n in range(8):
            product = dd_mul(weighted[n // 2], terms[n - n // 2])
            tiles = [(product[0][8 * i:8 * i + 8], product[1][8 * i:8 * i + 8]) for i in range(4)]
            sums.append(dd_add(dd_add(tiles[0], tiles[1]), dd_add(tiles[2], tiles[3])))

        def fold(a, b, near_mask, step):
            def one(i):
                x, y = a[i], b[i]
                far = jnp.where(near_mask, pltpu.roll(x, 8 - step, 0), pltpu.roll(y, step, 0))
                return jnp.where(near_mask, x, y), far
            kept, far = zip(*(one(i) for i in range(2)))
            return dd_add(kept, far)

        level = [fold(sums[2 * i], sums[2 * i + 1], sub < 4, 4) for i in range(4)]
        level = [fold(level[2 * i], level[2 * i + 1], sub % 4 < 2, 2) for i in range(2)]
        level = fold(level[0], level[1], sub % 2 < 1, 1)
        parts = [x.T for x in level]
        parts = [tuple(p[8 * i:8 * i + 8] for p in parts) for i in range(16)]
        while len(parts) > 1:
            parts = [dd_add(parts[i], parts[i + 1]) for i in range(0, len(parts), 2)]
        level = parts[0]
        for step in (4, 2, 1):
            level = dd_add(tuple(p[:step] for p in level), tuple(p[step:2 * step] for p in level))
        partial[0:1, 0:8] = level[0]
        partial[1:2, 0:8] = level[1]

        pl.semaphore_wait(ready, len(relay))
        for j, peer in enumerate(line_peer):
            remote(partial, gather_a.at[j], 5, peer).start()
        for d in (N, S):
            rows_copy(d, 1).start()
        surf_copy(NE, (2, 1), surf_b.at[pl.ds(5, 1)], 8).start()
        surf_copy(NW, (2, 1), surf_b.at[pl.ds(4, 1)], 8).start()
        surf_copy(SW, (0, 1), surf_b.at[pl.ds(3, 1)], 8).start()
        surf_copy(W, (0, 3), surf_b.at[pl.ds(0, 3)], 8).start()
        for d in (NE, NW, SE, SW):
            corner_copy(d).start()
        for d in (E, W):
            edge_copy(d).start()

        def total(own, others, number):
            parts = [(own[0:1], own[1:2])] + [(others[j, 0:1], others[j, 1:2]) for j in range(number)]
            while len(parts) > 1:
                parts = [dd_add(parts[i], parts[i + 1]) if i + 1 < len(parts) else parts[i]
                         for i in range(0, len(parts), 2)]
            return parts[0]

        wait_all(recv_sem, 1)
        wait_all(recv_sem, 7)
        south_count, north_count = surf_s[0, 0] * has_south, from_north(0, 0)
        count_own = jnp.concatenate([surf[t, 0] for t in range(3)] + [jnp.where(sub < 4, north_count, south_count)], 0)

        def with_rows(f, block, north, south):
            up = pltpu.roll(north, (8 - 2 * f) % 8, 0) if f else north
            down = pltpu.roll(south, 6 - 2 * f, 0) if f < 3 else south
            return jnp.concatenate([block, jnp.where(sub < 4, up, down)], 0)

        def main(k, slot, rows_in, base):
            active = jnp.where(count_own > k.astype(F32), 1.0, 0.0)
            north, south = rows_in[N - 2, k - base], rows_in[S - 2, k - base]
            quads = [with_rows(f, state[f, k], north, south) for f in range(4)]
            for f, value in enumerate(first_pass(active, quads, masked.at[slot], laps.at[k - base], weight.at[k - base])):
                tend[f, k] = value

        def finish(k, base):
            for f in range(4):
                tend[f, k] = tend[f, k] - second_pass(f, laps.at[k - base], weight.at[k - base])

        def unrolled(body, first, last, by):
            def step(i, carry):
                for j in range(by):
                    body(first + i * by + j, j)
                return carry
            lax.fori_loop(0, (last - first) // by, step, 0)

        unrolled(lambda k, slot: main(k, slot, rows_a, 0), 0, half, UNROLL)
        unrolled(lambda k, slot: finish(k, 0), 0, half, FINISH)

        wait_all(recv_sem, 5)
        hi, lo = total(partial, gather_a, nline - 1)
        mid[0:1] = hi
        mid[1:2] = lo
        for j, peer in enumerate(plane_peer):
            remote(mid, gather_b.at[j], 6, peer).start()

        wait_all(recv_sem, 2)
        unrolled(lambda k, slot: main(k, slot, rows_b, half), half, levels, UNROLL)
        unrolled(lambda k, slot: finish(k, half), half, levels, FINISH)
        wait_all(recv_sem, 8)
        depth = around_own(0)
        diag, vectors = krylov(depth, around_own(1), False)
        own_vectors = [quick(v[0][0][:24], v[0][1][:24]) for v in vectors]
        own_diag = diag[0][:24]
        count_side = jnp.concatenate([depth[1][:24], jnp.where(sub < 4, depth[1][24:32], depth[1][32:40])], 0)
        lane32 = iota((32, 128), 1)

        def spread(first, second):
            x = jnp.where(lane32 < 8, jnp.where(lane32 < 4, pltpu.roll(first, 4, 1), pltpu.roll(second, 4, 1)), 0.0)
            for step in (8, 16, 32, 64):
                x = x + pltpu.roll(x, step, 1)
            return x

        counts[0] = spread(count_side, count_own)
        counts[1] = spread(count_own, count_side)

        wait_all(recv_sem, 3)
        wait_all(recv_sem, 4)
        left24, left8 = lane24 % 8 < 4, lane % 8 < 4

        def edge_active(side, g):
            return jnp.where(counts[side] > (lane32 // 8 + g * GROUP).astype(F32), 1.0, 0.0)

        def edge_first(g, side, slot):
            if side == 0:
                north = jnp.where(left8, corners_in[NW - 4, g], rows_b[N - 2, levels - half + g])
                south = jnp.where(left8, corners_in[SW - 4, g], rows_b[S - 2, levels - half + g])
                blocks = [jnp.where(left24, edges_in[W, f, g], edges[f, g]) for f in range(4)]
            else:
                north = jnp.where(left8, rows_b[N - 2, levels - half + g], corners_in[NE - 4, g])
                south = jnp.where(left8, rows_b[S - 2, levels - half + g], corners_in[SE - 4, g])
                blocks = [jnp.where(left24, edges[f, g], edges_in[E, f, g]) for f in range(4)]
            quads = [with_rows(f, blocks[f], north, south) for f in range(4)]
            at = 2 * g + side
            return first_pass(edge_active(side, g), quads, masked.at[slot], laps.at[at], weight.at[at])

        def edge(g):
            west, east = edge_first(g, 0, 0), edge_first(g, 1, 1)
            for f in range(4):
                edge_out[f, g] = jnp.where(left24, east[f], west[f])

        def edge_finish(g):
            for f in range(4):
                west, east = (second_pass(f, laps.at[2 * g + i], weight.at[2 * g + i]) for i in range(2))
                edge_out[f, g] = edge_out[f, g] - jnp.where(left24, east, west)

        unrolled(lambda g, slot: edge(g), 0, groups, 1)
        unrolled(lambda g, slot: edge_finish(g), 0, groups, groups)

        rim = (lane24 < 2) | (lane24 >= 126)

        for k in range(levels):
            g, back = k // GROUP, (252 - 8 * (k % GROUP)) % 128
            for f in range(4):
                pltpu.store(tend.at[f, k], pltpu.roll(edge_out[f, g], back, 1), mask=rim)

        wait_all(recv_sem, 6)
        level = total(mid, gather_b, nplane - 1)

        def scalar(a, n):
            return jnp.broadcast_to(a[0:1, n:n + 1], (8, 128))

        mu = []
        for n in range(8):
            at = 4 * (n % 2) + 2 * (n // 2 % 2) + n // 4
            mu.append((scalar(level[0], at), scalar(level[1], at)))
        x_poly, r_poly = cg_coefficients(mu)
        for t in range(3):
            rows = slice(8 * t, 8 * t + 8)
            basis = [(v[0][rows], v[1][rows]) for v in own_vectors]

            def combined(poly):
                parts = [dd_mul(c, b) for c, b in zip(poly, basis)]
                while len(parts) > 1:
                    parts = [dd_add(parts[i], parts[i + 1]) if i + 1 < len(parts) else parts[i]
                             for i in range(0, len(parts), 2)]
                return parts[0]

            height = combined(x_poly)
            x_ref[rows] = (height[0] + height[1]) * (40.0 / 65536.0)
            rest = combined(r_poly)
            d = own_diag[rows]
            r_ref[rows] = (d * rest[0] + d * rest[1]) * (1.0 / 65536.0)

        for i in range(9):
            wait_all(send_sem, i)

        @pl.when(lat > 0)
        def _():
            wait_all(send_sem, 9)


    scratch = [
        pltpu.VMEM((24, 128), F32), pltpu.VMEM((24, 128), jnp.int32), pltpu.VMEM((24, 128), jnp.int32),
        pltpu.VMEM((4, levels, 24, 128), F32),
        pltpu.VMEM((3, 2, 8, 128), F32), pltpu.VMEM((3, 2, 8, 128), F32),
        pltpu.VMEM((1, 2, 8, 128), F32), pltpu.VMEM((6, 2, 8, 128), F32), pltpu.VMEM((4, 2, 8, 128), F32),
        pltpu.VMEM((4, groups, 24, 128), F32), pltpu.VMEM((2, 4, groups, 24, 128), F32),
        pltpu.VMEM((entries, 8, 128), F32), pltpu.VMEM((entries, 8, 128), F32),
        pltpu.VMEM((2, half, 8, 128), F32), pltpu.VMEM((2, entries - half, 8, 128), F32),
        pltpu.VMEM((4, groups, 8, 128), F32),
        pltpu.VMEM((2, 32, 128), F32), pltpu.VMEM((UNROLL, 4, 48, 128), F32),
        pltpu.VMEM((half, 4, 40, 128), F32), pltpu.VMEM((half, 24, 128), F32),
        pltpu.VMEM((4, groups, 24, 128), F32),
        pltpu.VMEM((2, 128), F32), pltpu.VMEM((nline - 1, 2, 128), F32),
        pltpu.VMEM((2, 128), F32), pltpu.VMEM((nplane - 1, 2, 128), F32),
        pltpu.SemaphoreType.DMA((5,)), pltpu.SemaphoreType.DMA((10,)), pltpu.SemaphoreType.DMA((10,)),
        pltpu.SemaphoreType.REGULAR,
    ]
    return kernel, scratch


def hand_out(x_ref, r_ref, tend_ref, x_out, r_out, tend_out, sem):
    copies = [pltpu.make_async_copy(tend_ref.at[f], tend_out.at[f], sem.at[f]) for f in range(4)]
    copies += [pltpu.make_async_copy(x_ref, x_out, sem.at[4]), pltpu.make_async_copy(r_ref, r_out, sem.at[5])]
    for copy in copies:
        copy.start()
    for copy in copies:
        copy.wait()


def solution(mesh):
    nlon, nlat = mesh.shape["lon"], mesh.shape["lat"]
    nplane = nlon // CORES
    nx = max(n for n in range(1, nplane + 1) if nplane % n == 0 and n * n <= nplane)
    ny = nplane // nx
    finer = Mesh(mesh.devices.reshape(nx, ny, CORES, nlat), ("x", "y", "core", "lat"))

    def per_device(surface_forcing, sea_mask, level_count, state):
        kernel, scratch = make_kernel(nx, ny, nlat, state.shape[1])
        results = pl.pallas_call(
            kernel,
            out_shape=(
                pltpu.VMEM(surface_forcing.shape, F32),
                pltpu.VMEM(surface_forcing.shape, F32),
                pltpu.VMEM(state.shape, F32),
            ),
            in_specs=[pl.BlockSpec(memory_space=pl.ANY)] * 4,
            out_specs=(
                pl.BlockSpec(memory_space=pltpu.VMEM),
                pl.BlockSpec(memory_space=pltpu.VMEM),
                pl.BlockSpec(memory_space=pltpu.VMEM),
            ),
            scratch_shapes=scratch,
            compiler_params=pltpu.CompilerParams(collective_id=0, has_side_effects=True, vmem_limit_bytes=65_030_000),
            name="ocean",
        )(surface_forcing, sea_mask, level_count, state)
        return pl.pallas_call(
            hand_out,
            out_shape=tuple(jax.ShapeDtypeStruct(r.shape, F32) for r in results),
            in_specs=[pl.BlockSpec(memory_space=pltpu.VMEM)] * 3,
            out_specs=[pl.BlockSpec(memory_space=pl.ANY)] * 3,
            scratch_shapes=[pltpu.SemaphoreType.DMA((6,))],
            compiler_params=pltpu.CompilerParams(vmem_limit_bytes=8 * 2**20),
            name="hand_out",
        )(*results)

    flat, deep = P("lat", ("x", "y", "core")), P(None, None, "lat", ("x", "y", "core"))
    return jax.shard_map(
        per_device, mesh=finer, in_specs=(flat, flat, flat, deep), out_specs=(flat, flat, deep), check_vma=False
    )
```

```python
import jax
import jax.numpy as jnp
from jax import lax
from jax.experimental import pallas as pl
from jax.experimental.pallas import tpu as pltpu
from jax.sharding import Mesh
from jax.sharding import PartitionSpec as P

MESH = pl.DeviceIdType.MESH
F32 = jnp.float32
CORES = 2
GROUP = 16
VISC = 0.02
HALO = 5
UNROLL = 2
FINISH = 4
DIRS = ((1, 0), (-1, 0), (0, 1), (0, -1), (1, 1), (-1, -1), (1, -1), (-1, 1))
OPP = (1, 0, 3, 2, 5, 4, 7, 6)
E, W, N, S, NE, SW, SE, NW = range(8)


def two_sum(a, b):
    s = a + b
    t = s - a
    return s, (a - (s - t)) + (b - t)


def quick(a, b):
    s = a + b
    return s, b - (s - a)


def split(a):
    t = 4097.0 * a
    h = t - (t - a)
    return h, a - h


def two_prod(a, b):
    p = a * b
    ah, al = split(a)
    bh, bl = split(b)
    return p, ((ah * bh - p) + ah * bl + al * bh) + al * bl


def short(hi, lo):
    t = 257.0 * hi
    h = t - (t - hi)
    return h, (hi - h) + lo


def dd_add(a, b):
    s, e = two_sum(a[0], b[0])
    return quick(s, e + (a[1] + b[1]))


def dd_mul(a, b):
    p, e = two_prod(a[0], b[0])
    return p, e + (a[0] * b[1] + a[1] * b[0])


def dd_neg(a):
    return -a[0], -a[1]


def dd_div(a, b, r):
    q = a[0] * r
    p, e = two_prod(q, b[0])
    rest = ((a[0] - p) - e) + (a[1] - q * b[1])
    return q, rest * r


def iota(shape, dim):
    return lax.broadcasted_iota(jnp.int32, shape, dim)


def shift_rows(x, step):
    return pltpu.roll(x, (-step) % x.shape[0], 0)


def shift_lanes(x, step):
    return pltpu.roll(x, (-step) % 128, 1)


def cg_coefficients(mu):
    s, t = dict(enumerate(mu)), dict(enumerate(mu))
    one = (jnp.ones_like(mu[0][0]), jnp.zeros_like(mu[0][0]))
    p, q = [one], [one]
    x = []
    for k in range(4):
        inverse = 1.0 / t[k + 1][0]
        alpha = dd_div(s[k], t[k + 1], inverse)
        minus = dd_neg(alpha)
        x = [dd_add(x[i], dd_mul(alpha, q[i])) if i < len(x) else dd_mul(alpha, q[i]) for i in range(k + 1)]
        moved = [dd_mul(minus, c) for c in q]
        p = [p[i] if i == 0 else (dd_add(p[i], moved[i - 1]) if i <= k else moved[i - 1]) for i in range(k + 2)]
        if k < 3:
            last = 6 - k
            s_next = {j: dd_add(s[j], dd_mul(minus, t[j + 1])) for j in range(k + 1, last + 1)}
            beta = dd_div(dd_neg(s_next[k + 1]), t[k + 1], inverse)
            t = {j: dd_add(s_next[j], dd_mul(beta, t[j])) for j in range(k + 2, last + 1)}
            s = s_next
            q = [dd_add(p[i], dd_mul(beta, q[i])) if i <= k else p[i] for i in range(k + 2)]
    return x, p


def first_pass(active, quads, masked, laps, weight):
    own = slice(0, 24)
    face_e, face_w = active * shift_lanes(active, 1), active * shift_lanes(active, -1)
    face_n, face_s = active * shift_rows(active, 1), active * shift_rows(active, -1)
    count = (face_e + face_w) + (face_n + face_s)
    weight[...] = VISC * active[own]
    visc_count = VISC * count[own]
    near = []
    for f, q in enumerate(quads):
        q = active * q
        masked[f, 0:8] = q[24:32]
        masked[f, 8:40] = q
        masked[f, 40:48] = q[0:8]
        near.append((q, shift_lanes(q, 1), shift_lanes(q, -1)))
    u, ue, uw = (x[own] for x in near[2])
    v = near[3][0][own]
    flow_e = (0.25 * face_e[own]) * (u + ue)
    flow_w = (0.25 * face_w[own]) * (u + uw)
    flow_n = (0.25 * face_n[own]) * (v + masked[3, 9:33])
    flow_s = (0.25 * face_s[own]) * (v + masked[3, 7:31])
    net = (flow_e - flow_w) + (flow_n - flow_s)
    out = []
    for f, (q, qe, qw) in enumerate(near):
        qn, qs = masked[f, 9:41], masked[f, 7:39]
        lap = active * ((qe + qw) + (qn + qs)) - count * q
        laps[f, 0:8] = lap[24:32]
        laps[f, 8:40] = lap
        flux = (net * q[own] + flow_e * qe[own]) + (flow_n * qn[own] - flow_w * qw[own]) - flow_s * qs[own]
        out.append(visc_count * lap[own] - flux)
    return out


def second_pass(f, laps, weight):
    lap = laps[f, 8:32]
    around = (shift_lanes(lap, 1) + shift_lanes(lap, -1)) + (laps[f, 9:33] + laps[f, 7:31])
    return weight[...] * around


def make_kernel(nx, ny, nlat, levels):
    nplane = nx * ny
    nline = CORES * nlat
    half = 4 * levels // 5
    quarter = half // 4 * 2
    groups = -(-levels // GROUP)
    entries = levels + groups
    def kernel(forcing_hbm, sea_hbm, count_hbm, state_hbm, x_ref, r_ref, tend,
               forcing, sea, count, state, surf, surf_in, surf_s, surf_b, surf_n, edges, edges_in, rows_up, rows_down,
               rows_a, rows_b, rows_c, corners_in, counts, masked, laps, weight, edge_out, partial, gather_a, mid, gather_b, in_sem, send_sem, recv_sem, ready):
        x, y = lax.axis_index("x"), lax.axis_index("y")
        core, lat = lax.axis_index("core"), lax.axis_index("lat")

        small = [pltpu.make_async_copy(a, b, in_sem.at[i]) for i, (a, b) in
                 enumerate(((forcing_hbm, forcing), (sea_hbm, sea), (count_hbm, count)))]
        large = [pltpu.make_async_copy(state_hbm.at[pl.ds(2 * f, 2)], state.at[pl.ds(2 * f, 2)], in_sem.at[3 + f])
                 for f in range(2)]
        for copy in small + large:
            copy.start()

        flip = 1 - core
        y_east, y_west = y + core, y + ny - flip
        place = {
            1: (lax.rem(x + lax.div(y_east, ny), nx), lax.rem(y_east, ny), flip),
            -1: (lax.rem(x + nx - 1 + lax.div(y_west, ny), nx), lax.rem(y_west, ny), flip),
            0: (x, y, core),
        }
        row = {1: lax.rem(lat + 1, nlat), -1: lax.rem(lat + nlat - 1, nlat), 0: lat}
        near = [(*place[dx], row[dy]) for dx, dy in DIRS]

        def hops(step, size):
            return min(step, size - step)

        plane_steps = sorted(((i, j) for i in range(nx) for j in range(ny) if i or j),
                             key=lambda p: -hops(p[0], nx) - hops(p[1], ny))
        xs = [x] + [lax.rem(x + i, nx) for i in range(1, nx)]
        ys = [y] + [lax.rem(y + j, ny) for j in range(1, ny)]
        plane_peer = [(xs[i], ys[j], core, lat) for i, j in plane_steps]
        line_steps = sorted(((c, j) for c in range(CORES) for j in range(nlat) if c or j),
                            key=lambda p: -hops(p[1], nlat))
        lats = [lat] + [lax.rem(lat + j, nlat) for j in range(1, nlat)]
        line_peer = [(x, y, (core, flip)[c], lats[j]) for c, j in line_steps]
        barrier = pltpu.get_barrier_semaphore()
        column = [(x, p, core, lat) for p in ys[1:]]
        rows = [(p, y, core, lat) for p in xs[1:]]
        along = [(x, y, c, lax.rem(lat + j, nlat)) for j in (2, nlat - 2, 1, nlat - 1) for c in (core, flip)]
        relay = column + [(x, y, core, lax.rem(lat + j, nlat)) for j in (2, nlat - 2)]
        peers = [near[NW], near[W]] + along[:4] + column + rows + along[4:] + [near[N], (x, y, flip, lat)]
        for peer in peers:
            pl.semaphore_signal(barrier, inc=1, device_id=peer, device_id_type=MESH)

        lane = iota((8, 128), 1)
        sub = iota((8, 128), 0)

        for copy in small:
            copy.wait()
        wet = sea[...] * count[...]
        for t in range(3):
            rows = slice(8 * t, 8 * t + 8)
            surf[t, 0] = wet[rows].astype(F32)
            surf[t, 1] = (sea[rows].astype(F32) * forcing[rows]) * 65536.0

        partial[...] = jnp.zeros_like(partial)
        mid[...] = jnp.zeros_like(mid)
        pl.semaphore_wait(barrier, len(peers))

        def remote(source, target, i, peer):
            return pltpu.make_async_remote_copy(source, target, send_sem.at[i], recv_sem.at[i],
                                                device_id=peer, device_id_type=MESH)

        def surf_copy(d, tiles, target, group):
            return remote(surf.at[pl.ds(*tiles)], target, group, near[d])

        def rows_copy(d, part):
            source = rows_up if DIRS[d][1] > 0 else rows_down
            span = (pl.ds(0, quarter), pl.ds(half, entries - half), pl.ds(quarter, half - quarter))[part]
            target = (rows_a, rows_b, rows_c)[part].at[OPP[d] - 2]
            return remote(source.at[span], target, (1, 2, 10)[part], near[d])

        def corner_copy(d):
            source = rows_up if DIRS[d][1] > 0 else rows_down
            return remote(source.at[pl.ds(levels, groups)], corners_in.at[OPP[d] - 4], 3, near[d])

        def edge_copy(d):
            return remote(edges, edges_in.at[OPP[d]], 4, near[d])

        landing = (surf_in, rows_a, rows_b, corners_in, edges_in, gather_a, gather_b, surf_s, surf_b, surf_n, rows_c)

        def wait_all(sem, i):
            pltpu.make_async_copy(landing[i], landing[i], sem.at[i]).wait()

        southward = (surf_copy(SE, (0, 2), surf_n.at[pl.ds(2, 2)], 9), surf_copy(S, (0, 2), surf_n.at[pl.ds(0, 2)], 9))

        @pl.when(lat > 0)
        def _():
            southward[0].start()

        surf_copy(E, (0, 3), surf_in, 0).start()

        @pl.when(lat > 0)
        def _():
            southward[1].start()

        surf_copy(N, (2, 1), surf_s, 7).start()
        for peer in relay:
            pl.semaphore_signal(ready, inc=1, device_id=peer, device_id_type=MESH)
        for copy in large:
            copy.wait()

        lane24 = iota((24, 128), 1)

        def pack_edges(f, carry):
            for g in range(groups):
                packed = jnp.zeros((24, 128), F32)
                for i in range(min(GROUP, levels - g * GROUP)):
                    moved = pltpu.roll(state[f, g * GROUP + i], (4 + 8 * i) % 128, 1)
                    packed = jnp.where(lane24 // 8 == i, moved, packed)
                edges[f, g] = packed
            return carry


        def packed_rows(tile_of):
            up, down = None, None
            for f in range(4):
                top = pltpu.roll(tile_of(f, slice(16, 24)), (2 * f + 2) % 8, 0)
                low = tile_of(f, slice(0, 8))
                low = pltpu.roll(low, 2 * f, 0) if f else low
                up = top if f == 0 else jnp.where(sub // 2 == f, top, up)
                down = low if f == 0 else jnp.where(sub // 2 == f, low, down)
            return up, down

        def pack_rows(k, carry):
            up, down = packed_rows(lambda f, rows: state[f, k, rows])
            rows_up[k] = up
            rows_down[k] = down
            return carry

        lax.fori_loop(0, levels, pack_rows, 0)
        for part in (0, 2):
            for d in (N, S):
                rows_copy(d, part).start()
        lax.fori_loop(0, 4, pack_edges, 0)
        for g in range(groups):
            up, down = packed_rows(lambda f, rows: edges[f, g, rows])
            rows_up[levels + g] = up
            rows_down[levels + g] = down

        wait_all(recv_sem, 0)

        @pl.when(lat < nlat - 1)
        def _():
            wait_all(recv_sem, 9)


        has_south = jnp.where(lat > 0, 1.0, 0.0).astype(F32)

        def from_north(tile, v):
            return jnp.where(lat < nlat - 1, surf_n[tile, v], 0.0)

        def ahead(v):
            own = [surf[t, v] for t in range(3)] + [from_north(t, v) for t in range(2)]
            west = [surf_in[t, v] for t in range(3)] + [from_north(2 + t, v) for t in range(2)]
            return jnp.concatenate(own, 0), jnp.concatenate(west, 0)

        def around_own(v):
            own = [surf[t, v] for t in range(3)] + [from_north(0, v), surf_s[0, v] * has_south]
            side = [jnp.where(lane < 64, surf_b[t, v], surf_in[t, v]) for t in range(3)]
            side.append(jnp.where(lane < 64, jnp.where(lat < nlat - 1, surf_b[3, v], 0.0), from_north(2, v)))
            side.append(jnp.where(lane < 64, surf_b[4, v], surf_b[5, v]) * has_south)
            return jnp.concatenate(own, 0), jnp.concatenate(side, 0)

        lane40 = iota((40, 128), 1)

        def to_east(pair):
            a, b = shift_lanes(pair[0], 1), shift_lanes(pair[1], 1)
            last = iota(a.shape, 1) == 127
            return jnp.where(last, b, a), jnp.where(last, a, b)

        def to_west(pair):
            a, b = shift_lanes(pair[0], -1), shift_lanes(pair[1], -1)
            first = iota(a.shape, 1) == 0
            return jnp.where(first, b, a), jnp.where(first, a, b)

        def to_north(pair):
            return shift_rows(pair[0], 1), shift_rows(pair[1], 1)

        def to_south(pair):
            return shift_rows(pair[0], -1), shift_rows(pair[1], -1)

        moves = (to_east, to_west, to_north, to_south)
        def krylov(depth, force, both, cut=None, kept=40):
            moved = [move(depth) for move in moves]
            faces = [[jnp.minimum(depth[t], m[t]) for m in moved] for t in range(2)]
            if cut is not None:
                faces = [[e, w, n, s * cut] for e, w, n, s in faces]
            diag = [2.0 + ((faces[t][0] + faces[t][1]) + (faces[t][2] + faces[t][3])) for t in range(2)]
            inverse = [1.0 / diag[t] for t in range(2)]

            def over_diag(hi, lo, t):
                q, _ = short(hi * inverse[t], 0.0)
                return q, ((hi - diag[t] * q) + lo) * inverse[t]

            vectors = [[short(*over_diag(force[t], 0.0, t)) for t in range(2)]]
            for k in range(4):
                last = vectors[-1]
                high = [move((last[0][0], last[1][0])) for move in moves]
                low = [move((last[0][1], last[1][1])) for move in moves]
                if k == 0 and kept < 40:
                    high, low = ([[x[:kept] for x in pair] for pair in part] for part in (high, low))
                    last = [tuple(x[:kept] for x in pair) for pair in last]
                    faces = [[x[:kept] for x in part] for part in faces]
                    diag, inverse = [x[:kept] for x in diag], [x[:kept] for x in inverse]
                following = []
                for t in range(2 if both or k < 3 else 1):
                    terms = [faces[t][i] * high[i][t] for i in range(4)]
                    fine = [faces[t][i] * low[i][t] for i in range(4)]
                    s0, e0 = two_sum(terms[0], terms[1])
                    s1, e1 = two_sum(terms[2], terms[3])
                    s, e2 = two_sum(s0, s1)
                    rest = ((e0 + e1) + e2) + ((fine[0] + fine[1]) + (fine[2] + fine[3]))
                    q, q_low = over_diag(s, rest, t)
                    s, e = two_sum(last[t][0], -q)
                    following.append(short(s, e + (last[t][1] - q_low)))
                vectors.append(following)
            return diag, vectors

        def counted(pair):
            cells = jnp.where(iota(pair[0].shape, 1) < 128 - HALO, pair[0], pair[1])
            first = jnp.where(sub < HALO, cells[24:32], cells[0:8])
            return jnp.concatenate([first, cells[8:24], jnp.where(sub < southern, cells[0:8], 0.0)], 0)

        southern = jnp.where(lat > 0, 0, HALO)
        cut = jnp.where(iota((40, 128), 0) == 0, has_south, 1.0)
        diag, vectors = krylov(ahead(0), ahead(1), True, cut, 32)
        terms = [tuple(counted((v[0][i], v[1][i])) for i in range(2)) for v in vectors]
        scale = counted(diag)
        weighted = [quick(scale * hi, scale * lo) for hi, lo in terms[:4]]
        terms = [quick(hi, lo) for hi, lo in terms]

        sums = []
        for n in range(8):
            product = dd_mul(weighted[n // 2], terms[n - n // 2])
            tiles = [(product[0][8 * i:8 * i + 8], product[1][8 * i:8 * i + 8]) for i in range(4)]
            sums.append(dd_add(dd_add(tiles[0], tiles[1]), dd_add(tiles[2], tiles[3])))

        def fold(a, b, near_mask, step):
            def one(i):
                x, y = a[i], b[i]
                far = jnp.where(near_mask, pltpu.roll(x, 8 - step, 0), pltpu.roll(y, step, 0))
                return jnp.where(near_mask, x, y), far
            kept, far = zip(*(one(i) for i in range(2)))
            return dd_add(kept, far)

        level = [fold(sums[2 * i], sums[2 * i + 1], sub < 4, 4) for i in range(4)]
        level = [fold(level[2 * i], level[2 * i + 1], sub % 4 < 2, 2) for i in range(2)]
        level = fold(level[0], level[1], sub % 2 < 1, 1)
        parts = [x.T for x in level]
        parts = [tuple(p[8 * i:8 * i + 8] for p in parts) for i in range(16)]
        while len(parts) > 1:
            parts = [dd_add(parts[i], parts[i + 1]) for i in range(0, len(parts), 2)]
        level = parts[0]
        for step in (4, 2, 1):
            level = dd_add(tuple(p[:step] for p in level), tuple(p[step:2 * step] for p in level))
        partial[0:1, 0:8] = level[0]
        partial[1:2, 0:8] = level[1]

        pl.semaphore_wait(ready, len(relay))
        for j, peer in enumerate(line_peer):
            remote(partial, gather_a.at[j], 5, peer).start()
        for d in (N, S):
            rows_copy(d, 1).start()
        surf_copy(NE, (2, 1), surf_b.at[pl.ds(5, 1)], 8).start()
        surf_copy(NW, (2, 1), surf_b.at[pl.ds(4, 1)], 8).start()
        surf_copy(SW, (0, 1), surf_b.at[pl.ds(3, 1)], 8).start()
        surf_copy(W, (0, 3), surf_b.at[pl.ds(0, 3)], 8).start()
        for d in (NE, NW, SE, SW):
            corner_copy(d).start()
        for d in (E, W):
            edge_copy(d).start()

        def total(own, others, number):
            parts = [(own[0:1], own[1:2])] + [(others[j, 0:1], others[j, 1:2]) for j in range(number)]
            while len(parts) > 1:
                parts = [dd_add(parts[i], parts[i + 1]) if i + 1 < len(parts) else parts[i]
                         for i in range(0, len(parts), 2)]
            return parts[0]

        wait_all(recv_sem, 1)
        wait_all(recv_sem, 7)
        south_count, north_count = surf_s[0, 0] * has_south, from_north(0, 0)
        count_own = jnp.concatenate([surf[t, 0] for t in range(3)] + [jnp.where(sub < 4, north_count, south_count)], 0)

        def with_rows(f, block, north, south):
            up = pltpu.roll(north, (8 - 2 * f) % 8, 0) if f else north
            down = pltpu.roll(south, 6 - 2 * f, 0) if f < 3 else south
            return jnp.concatenate([block, jnp.where(sub < 4, up, down)], 0)

        def main(k, slot, rows_in, first, base):
            active = jnp.where(count_own > k.astype(F32), 1.0, 0.0)
            north, south = rows_in[N - 2, k - first], rows_in[S - 2, k - first]
            quads = [with_rows(f, state[f, k], north, south) for f in range(4)]
            for f, value in enumerate(first_pass(active, quads, masked.at[slot], laps.at[k - base], weight.at[k - base])):
                tend[f, k] = value

        def finish(k, base):
            for f in range(4):
                tend[f, k] = tend[f, k] - second_pass(f, laps.at[k - base], weight.at[k - base])

        def unrolled(body, first, last, by):
            def step(i, carry):
                for j in range(by):
                    body(first + i * by + j, j)
                return carry
            lax.fori_loop(0, (last - first) // by, step, 0)

        unrolled(lambda k, slot: main(k, slot, rows_a, 0, 0), 0, quarter, UNROLL)
        wait_all(recv_sem, 10)
        unrolled(lambda k, slot: main(k, slot, rows_c, quarter, 0), quarter, half, UNROLL)
        unrolled(lambda k, slot: finish(k, 0), 0, half, FINISH)

        wait_all(recv_sem, 5)
        hi, lo = total(partial, gather_a, nline - 1)
        mid[0:1] = hi
        mid[1:2] = lo
        for j, peer in enumerate(plane_peer):
            remote(mid, gather_b.at[j], 6, peer).start()

        wait_all(recv_sem, 2)
        unrolled(lambda k, slot: main(k, slot, rows_b, half, half), half, levels, UNROLL)
        unrolled(lambda k, slot: finish(k, half), half, levels, FINISH)
        wait_all(recv_sem, 8)
        depth = around_own(0)
        diag, vectors = krylov(depth, around_own(1), False)
        own_vectors = [quick(v[0][0][:24], v[0][1][:24]) for v in vectors]
        own_diag = diag[0][:24]
        count_side = jnp.concatenate([depth[1][:24], jnp.where(sub < 4, depth[1][24:32], depth[1][32:40])], 0)
        lane32 = iota((32, 128), 1)

        def spread(first, second):
            x = jnp.where(lane32 < 8, jnp.where(lane32 < 4, pltpu.roll(first, 4, 1), pltpu.roll(second, 4, 1)), 0.0)
            for step in (8, 16, 32, 64):
                x = x + pltpu.roll(x, step, 1)
            return x

        counts[0] = spread(count_side, count_own)
        counts[1] = spread(count_own, count_side)

        wait_all(recv_sem, 3)
        wait_all(recv_sem, 4)
        left24, left8 = lane24 % 8 < 4, lane % 8 < 4

        def edge_active(side, g):
            return jnp.where(counts[side] > (lane32 // 8 + g * GROUP).astype(F32), 1.0, 0.0)

        def edge_first(g, side, slot):
            if side == 0:
                north = jnp.where(left8, corners_in[NW - 4, g], rows_b[N - 2, levels - half + g])
                south = jnp.where(left8, corners_in[SW - 4, g], rows_b[S - 2, levels - half + g])
                blocks = [jnp.where(left24, edges_in[W, f, g], edges[f, g]) for f in range(4)]
            else:
                north = jnp.where(left8, rows_b[N - 2, levels - half + g], corners_in[NE - 4, g])
                south = jnp.where(left8, rows_b[S - 2, levels - half + g], corners_in[SE - 4, g])
                blocks = [jnp.where(left24, edges[f, g], edges_in[E, f, g]) for f in range(4)]
            quads = [with_rows(f, blocks[f], north, south) for f in range(4)]
            at = 2 * g + side
            return first_pass(edge_active(side, g), quads, masked.at[slot], laps.at[at], weight.at[at])

        def edge(g):
            west, east = edge_first(g, 0, 0), edge_first(g, 1, 1)
            for f in range(4):
                edge_out[f, g] = jnp.where(left24, east[f], west[f])

        def edge_finish(g):
            for f in range(4):
                west, east = (second_pass(f, laps.at[2 * g + i], weight.at[2 * g + i]) for i in range(2))
                edge_out[f, g] = edge_out[f, g] - jnp.where(left24, east, west)

        unrolled(lambda g, slot: edge(g), 0, groups, 1)
        unrolled(lambda g, slot: edge_finish(g), 0, groups, groups)

        rim = (lane24 < 2) | (lane24 >= 126)

        for k in range(levels):
            g, back = k // GROUP, (252 - 8 * (k % GROUP)) % 128
            for f in range(4):
                pltpu.store(tend.at[f, k], pltpu.roll(edge_out[f, g], back, 1), mask=rim)

        wait_all(recv_sem, 6)
        level = total(mid, gather_b, nplane - 1)

        def scalar(a, n):
            return jnp.broadcast_to(a[0:1, n:n + 1], (8, 128))

        mu = []
        for n in range(8):
            at = 4 * (n % 2) + 2 * (n // 2 % 2) + n // 4
            mu.append((scalar(level[0], at), scalar(level[1], at)))
        x_poly, r_poly = cg_coefficients(mu)
        for t in range(3):
            rows = slice(8 * t, 8 * t + 8)
            basis = [(v[0][rows], v[1][rows]) for v in own_vectors]

            def combined(poly):
                parts = [dd_mul(c, b) for c, b in zip(poly, basis)]
                while len(parts) > 1:
                    parts = [dd_add(parts[i], parts[i + 1]) if i + 1 < len(parts) else parts[i]
                             for i in range(0, len(parts), 2)]
                return parts[0]

            height = combined(x_poly)
            x_ref[rows] = (height[0] + height[1]) * (40.0 / 65536.0)
            rest = combined(r_poly)
            d = own_diag[rows]
            r_ref[rows] = (d * rest[0] + d * rest[1]) * (1.0 / 65536.0)

        for i in (0, 1, 2, 3, 4, 5, 6, 7, 8, 10):
            wait_all(send_sem, i)

        @pl.when(lat > 0)
        def _():
            wait_all(send_sem, 9)


    scratch = [
        pltpu.VMEM((24, 128), F32), pltpu.VMEM((24, 128), jnp.int32), pltpu.VMEM((24, 128), jnp.int32),
        pltpu.VMEM((4, levels, 24, 128), F32),
        pltpu.VMEM((3, 2, 8, 128), F32), pltpu.VMEM((3, 2, 8, 128), F32),
        pltpu.VMEM((1, 2, 8, 128), F32), pltpu.VMEM((6, 2, 8, 128), F32), pltpu.VMEM((4, 2, 8, 128), F32),
        pltpu.VMEM((4, groups, 24, 128), F32), pltpu.VMEM((2, 4, groups, 24, 128), F32),
        pltpu.VMEM((entries, 8, 128), F32), pltpu.VMEM((entries, 8, 128), F32),
        pltpu.VMEM((2, quarter, 8, 128), F32), pltpu.VMEM((2, entries - half, 8, 128), F32),
        pltpu.VMEM((2, half - quarter, 8, 128), F32),
        pltpu.VMEM((4, groups, 8, 128), F32),
        pltpu.VMEM((2, 32, 128), F32), pltpu.VMEM((UNROLL, 4, 48, 128), F32),
        pltpu.VMEM((half, 4, 40, 128), F32), pltpu.VMEM((half, 24, 128), F32),
        pltpu.VMEM((4, groups, 24, 128), F32),
        pltpu.VMEM((2, 128), F32), pltpu.VMEM((nline - 1, 2, 128), F32),
        pltpu.VMEM((2, 128), F32), pltpu.VMEM((nplane - 1, 2, 128), F32),
        pltpu.SemaphoreType.DMA((5,)), pltpu.SemaphoreType.DMA((11,)), pltpu.SemaphoreType.DMA((11,)),
        pltpu.SemaphoreType.REGULAR,
    ]
    return kernel, scratch


def hand_out(x_ref, r_ref, tend_ref, x_out, r_out, tend_out, sem):
    copies = [pltpu.make_async_copy(tend_ref.at[f], tend_out.at[f], sem.at[f]) for f in range(4)]
    copies += [pltpu.make_async_copy(x_ref, x_out, sem.at[4]), pltpu.make_async_copy(r_ref, r_out, sem.at[5])]
    for copy in copies:
        copy.start()
    for copy in copies:
        copy.wait()


def solution(mesh):
    nlon, nlat = mesh.shape["lon"], mesh.shape["lat"]
    nplane = nlon // CORES
    nx = max(n for n in range(1, nplane + 1) if nplane % n == 0 and n * n <= nplane)
    ny = nplane // nx
    finer = Mesh(mesh.devices.reshape(nx, ny, CORES, nlat), ("x", "y", "core", "lat"))

    def per_device(surface_forcing, sea_mask, level_count, state):
        kernel, scratch = make_kernel(nx, ny, nlat, state.shape[1])
        results = pl.pallas_call(
            kernel,
            out_shape=(
                pltpu.VMEM(surface_forcing.shape, F32),
                pltpu.VMEM(surface_forcing.shape, F32),
                pltpu.VMEM(state.shape, F32),
            ),
            in_specs=[pl.BlockSpec(memory_space=pl.ANY)] * 4,
            out_specs=(
                pl.BlockSpec(memory_space=pltpu.VMEM),
                pl.BlockSpec(memory_space=pltpu.VMEM),
                pl.BlockSpec(memory_space=pltpu.VMEM),
            ),
            scratch_shapes=scratch,
            compiler_params=pltpu.CompilerParams(collective_id=0, has_side_effects=True, vmem_limit_bytes=65_030_000),
            name="ocean",
        )(surface_forcing, sea_mask, level_count, state)
        return pl.pallas_call(
            hand_out,
            out_shape=tuple(jax.ShapeDtypeStruct(r.shape, F32) for r in results),
            in_specs=[pl.BlockSpec(memory_space=pltpu.VMEM)] * 3,
            out_specs=[pl.BlockSpec(memory_space=pl.ANY)] * 3,
            scratch_shapes=[pltpu.SemaphoreType.DMA((6,))],
            compiler_params=pltpu.CompilerParams(vmem_limit_bytes=8 * 2**20),
            name="hand_out",
        )(*results)

    flat, deep = P("lat", ("x", "y", "core")), P(None, None, "lat", ("x", "y", "core"))
    return jax.shard_map(
        per_device, mesh=finer, in_specs=(flat, flat, flat, deep), out_specs=(flat, flat, deep), check_vma=False
    )
```

```python
import jax
import jax.numpy as jnp
from jax import lax
from jax.experimental import pallas as pl
from jax.experimental.pallas import tpu as pltpu
from jax.sharding import Mesh
from jax.sharding import PartitionSpec as P

MESH = pl.DeviceIdType.MESH
F32 = jnp.float32
CORES = 2
GROUP = 16
VISC = 0.02
HALO = 5
UNROLL = 2
FINISH = 8
DIRS = ((1, 0), (-1, 0), (0, 1), (0, -1), (1, 1), (-1, -1), (1, -1), (-1, 1))
OPP = (1, 0, 3, 2, 5, 4, 7, 6)
E, W, N, S, NE, SW, SE, NW = range(8)


def two_sum(a, b):
    s = a + b
    t = s - a
    return s, (a - (s - t)) + (b - t)


def quick(a, b):
    s = a + b
    return s, b - (s - a)


def split(a):
    t = 4097.0 * a
    h = t - (t - a)
    return h, a - h


def two_prod(a, b):
    p = a * b
    ah, al = split(a)
    bh, bl = split(b)
    return p, ((ah * bh - p) + ah * bl + al * bh) + al * bl


def short(hi, lo):
    t = 257.0 * hi
    h = t - (t - hi)
    return h, (hi - h) + lo


def dd_add(a, b):
    s, e = two_sum(a[0], b[0])
    return quick(s, e + (a[1] + b[1]))


def dd_mul(a, b):
    p, e = two_prod(a[0], b[0])
    return p, e + (a[0] * b[1] + a[1] * b[0])


def dd_neg(a):
    return -a[0], -a[1]


def dd_div(a, b, r):
    q = a[0] * r
    p, e = two_prod(q, b[0])
    rest = ((a[0] - p) - e) + (a[1] - q * b[1])
    return q, rest * r


def iota(shape, dim):
    return lax.broadcasted_iota(jnp.int32, shape, dim)


def shift_rows(x, step):
    return pltpu.roll(x, (-step) % x.shape[0], 0)


def shift_lanes(x, step):
    return pltpu.roll(x, (-step) % 128, 1)


def cg_coefficients(mu):
    s, t = dict(enumerate(mu)), dict(enumerate(mu))
    one = (jnp.ones_like(mu[0][0]), jnp.zeros_like(mu[0][0]))
    p, q = [one], [one]
    x = []
    for k in range(4):
        inverse = 1.0 / t[k + 1][0]
        alpha = dd_div(s[k], t[k + 1], inverse)
        minus = dd_neg(alpha)
        x = [dd_add(x[i], dd_mul(alpha, q[i])) if i < len(x) else dd_mul(alpha, q[i]) for i in range(k + 1)]
        moved = [dd_mul(minus, c) for c in q]
        p = [p[i] if i == 0 else (dd_add(p[i], moved[i - 1]) if i <= k else moved[i - 1]) for i in range(k + 2)]
        if k < 3:
            last = 6 - k
            s_next = {j: dd_add(s[j], dd_mul(minus, t[j + 1])) for j in range(k + 1, last + 1)}
            beta = dd_div(dd_neg(s_next[k + 1]), t[k + 1], inverse)
            t = {j: dd_add(s_next[j], dd_mul(beta, t[j])) for j in range(k + 2, last + 1)}
            s = s_next
            q = [dd_add(p[i], dd_mul(beta, q[i])) if i <= k else p[i] for i in range(k + 2)]
    return x, p


def first_pass(active, quads, masked, laps, weight):
    own = slice(0, 24)
    face_e, face_w = active * shift_lanes(active, 1), active * shift_lanes(active, -1)
    face_n, face_s = active * shift_rows(active, 1), active * shift_rows(active, -1)
    count = (face_e + face_w) + (face_n + face_s)
    weight[...] = VISC * active[own]
    visc_count = VISC * count[own]
    near = []
    for f, q in enumerate(quads):
        q = active * q
        masked[f, 0:8] = q[24:32]
        masked[f, 8:40] = q
        masked[f, 40:48] = q[0:8]
        near.append((q, shift_lanes(q, 1), shift_lanes(q, -1)))
    u, ue, uw = (x[own] for x in near[2])
    v = near[3][0][own]
    flow_e = (0.25 * face_e[own]) * (u + ue)
    flow_w = (0.25 * face_w[own]) * (u + uw)
    flow_n = (0.25 * face_n[own]) * (v + masked[3, 9:33])
    flow_s = (0.25 * face_s[own]) * (v + masked[3, 7:31])
    net = (flow_e - flow_w) + (flow_n - flow_s)
    out = []
    for f, (q, qe, qw) in enumerate(near):
        qn, qs = masked[f, 9:41], masked[f, 7:39]
        lap = active * ((qe + qw) + (qn + qs)) - count * q
        laps[f, 0:8] = lap[24:32]
        laps[f, 8:40] = lap
        flux = (net * q[own] + flow_e * qe[own]) + (flow_n * qn[own] - flow_w * qw[own]) - flow_s * qs[own]
        out.append(visc_count * lap[own] - flux)
    return out


def second_pass(f, laps, weight):
    lap = laps[f, 8:32]
    around = (shift_lanes(lap, 1) + shift_lanes(lap, -1)) + (laps[f, 9:33] + laps[f, 7:31])
    return weight[...] * around


def make_kernel(nx, ny, nlat, levels):
    nplane = nx * ny
    nline = CORES * nlat
    half = 4 * levels // 5
    quarter = half // 4 * 2
    groups = -(-levels // GROUP)
    entries = levels + groups
    def kernel(forcing_hbm, sea_hbm, count_hbm, state_hbm, x_ref, r_ref, tend,
               forcing, sea, count, state, surf, surf_in, surf_s, surf_b, surf_n, edges, edges_in, rows_up, rows_down,
               rows_a, rows_b, rows_c, corners_in, counts, masked, laps, weight, edge_out, partial, gather_a, mid, gather_b, in_sem, send_sem, recv_sem, ready):
        x, y = lax.axis_index("x"), lax.axis_index("y")
        core, lat = lax.axis_index("core"), lax.axis_index("lat")

        small = [pltpu.make_async_copy(a, b, in_sem.at[i]) for i, (a, b) in
                 enumerate(((forcing_hbm, forcing), (sea_hbm, sea), (count_hbm, count)))]
        large = [pltpu.make_async_copy(state_hbm.at[pl.ds(2 * f, 2)], state.at[pl.ds(2 * f, 2)], in_sem.at[3 + f])
                 for f in range(2)]
        for copy in small + large:
            copy.start()

        flip = 1 - core
        y_east, y_west = y + core, y + ny - flip
        place = {
            1: (lax.rem(x + lax.div(y_east, ny), nx), lax.rem(y_east, ny), flip),
            -1: (lax.rem(x + nx - 1 + lax.div(y_west, ny), nx), lax.rem(y_west, ny), flip),
            0: (x, y, core),
        }
        row = {1: lax.rem(lat + 1, nlat), -1: lax.rem(lat + nlat - 1, nlat), 0: lat}
        near = [(*place[dx], row[dy]) for dx, dy in DIRS]

        def hops(step, size):
            return min(step, size - step)

        plane_steps = sorted(((i, j) for i in range(nx) for j in range(ny) if i or j),
                             key=lambda p: -hops(p[0], nx) - hops(p[1], ny))
        xs = [x] + [lax.rem(x + i, nx) for i in range(1, nx)]
        ys = [y] + [lax.rem(y + j, ny) for j in range(1, ny)]
        plane_peer = [(xs[i], ys[j], core, lat) for i, j in plane_steps]
        line_steps = sorted(((c, j) for c in range(CORES) for j in range(nlat) if c or j),
                            key=lambda p: -hops(p[1], nlat))
        lats = [lat] + [lax.rem(lat + j, nlat) for j in range(1, nlat)]
        line_peer = [(x, y, (core, flip)[c], lats[j]) for c, j in line_steps]
        barrier = pltpu.get_barrier_semaphore()
        column = [(x, p, core, lat) for p in ys[1:]]
        rows = [(p, y, core, lat) for p in xs[1:]]
        along = [(x, y, c, lax.rem(lat + j, nlat)) for j in (2, nlat - 2, 1, nlat - 1) for c in (core, flip)]
        relay = column + [(x, y, core, lax.rem(lat + j, nlat)) for j in (2, nlat - 2)]
        peers = [near[NW], near[W]] + along[:4] + column + rows + along[4:] + [near[N], (x, y, flip, lat)]
        for peer in peers:
            pl.semaphore_signal(barrier, inc=1, device_id=peer, device_id_type=MESH)

        lane = iota((8, 128), 1)
        sub = iota((8, 128), 0)

        for copy in small:
            copy.wait()
        wet = sea[...] * count[...]
        for t in range(3):
            rows = slice(8 * t, 8 * t + 8)
            surf[t, 0] = wet[rows].astype(F32)
            surf[t, 1] = (sea[rows].astype(F32) * forcing[rows]) * 65536.0

        partial[...] = jnp.zeros_like(partial)
        mid[...] = jnp.zeros_like(mid)
        pl.semaphore_wait(barrier, len(peers))

        def remote(source, target, i, peer):
            return pltpu.make_async_remote_copy(source, target, send_sem.at[i], recv_sem.at[i],
                                                device_id=peer, device_id_type=MESH)

        def surf_copy(d, tiles, target, group):
            return remote(surf.at[pl.ds(*tiles)], target, group, near[d])

        def rows_copy(d, part):
            source = rows_up if DIRS[d][1] > 0 else rows_down
            span = (pl.ds(0, quarter), pl.ds(half, entries - half), pl.ds(quarter, half - quarter))[part]
            target = (rows_a, rows_b, rows_c)[part].at[OPP[d] - 2]
            return remote(source.at[span], target, (1, 2, 10)[part], near[d])

        def corner_copy(d):
            source = rows_up if DIRS[d][1] > 0 else rows_down
            return remote(source.at[pl.ds(levels, groups)], corners_in.at[OPP[d] - 4], 3, near[d])

        def edge_copy(d):
            return remote(edges, edges_in.at[OPP[d]], 4, near[d])

        landing = (surf_in, rows_a, rows_b, corners_in, edges_in, gather_a, gather_b, surf_s, surf_b, surf_n, rows_c)

        def wait_all(sem, i):
            pltpu.make_async_copy(landing[i], landing[i], sem.at[i]).wait()

        southward = (surf_copy(SE, (0, 2), surf_n.at[pl.ds(2, 2)], 9), surf_copy(S, (0, 2), surf_n.at[pl.ds(0, 2)], 9))

        @pl.when(lat > 0)
        def _():
            southward[0].start()

        surf_copy(E, (0, 3), surf_in, 0).start()

        @pl.when(lat > 0)
        def _():
            southward[1].start()

        surf_copy(N, (2, 1), surf_s, 7).start()
        for peer in relay:
            pl.semaphore_signal(ready, inc=1, device_id=peer, device_id_type=MESH)
        for copy in large:
            copy.wait()

        lane24 = iota((24, 128), 1)

        def pack_edges(f, carry):
            for g in range(groups):
                packed = jnp.zeros((24, 128), F32)
                for i in range(min(GROUP, levels - g * GROUP)):
                    moved = pltpu.roll(state[f, g * GROUP + i], (4 + 8 * i) % 128, 1)
                    packed = jnp.where(lane24 // 8 == i, moved, packed)
                edges[f, g] = packed
            return carry


        def packed_rows(tile_of):
            up, down = None, None
            for f in range(4):
                top = pltpu.roll(tile_of(f, slice(16, 24)), (2 * f + 2) % 8, 0)
                low = tile_of(f, slice(0, 8))
                low = pltpu.roll(low, 2 * f, 0) if f else low
                up = top if f == 0 else jnp.where(sub // 2 == f, top, up)
                down = low if f == 0 else jnp.where(sub // 2 == f, low, down)
            return up, down

        def pack_rows(k, carry):
            up, down = packed_rows(lambda f, rows: state[f, k, rows])
            rows_up[k] = up
            rows_down[k] = down
            return carry

        lax.fori_loop(0, levels, pack_rows, 0)
        for part in (0, 2):
            for d in (N, S):
                rows_copy(d, part).start()
        lax.fori_loop(0, 4, pack_edges, 0)
        for g in range(groups):
            up, down = packed_rows(lambda f, rows: edges[f, g, rows])
            rows_up[levels + g] = up
            rows_down[levels + g] = down

        wait_all(recv_sem, 0)

        @pl.when(lat < nlat - 1)
        def _():
            wait_all(recv_sem, 9)


        has_south = jnp.where(lat > 0, 1.0, 0.0).astype(F32)

        def from_north(tile, v):
            return jnp.where(lat < nlat - 1, surf_n[tile, v], 0.0)

        def ahead(v):
            own = [surf[t, v] for t in range(3)] + [from_north(t, v) for t in range(2)]
            west = [surf_in[t, v] for t in range(3)] + [from_north(2 + t, v) for t in range(2)]
            return jnp.concatenate(own, 0), jnp.concatenate(west, 0)

        def around_own(v):
            own = [surf[t, v] for t in range(3)] + [from_north(0, v), surf_s[0, v] * has_south]
            side = [jnp.where(lane < 64, surf_b[t, v], surf_in[t, v]) for t in range(3)]
            side.append(jnp.where(lane < 64, jnp.where(lat < nlat - 1, surf_b[3, v], 0.0), from_north(2, v)))
            side.append(jnp.where(lane < 64, surf_b[4, v], surf_b[5, v]) * has_south)
            return jnp.concatenate(own, 0), jnp.concatenate(side, 0)

        lane40 = iota((40, 128), 1)

        def to_east(pair):
            a, b = shift_lanes(pair[0], 1), shift_lanes(pair[1], 1)
            last = iota(a.shape, 1) == 127
            return jnp.where(last, b, a), jnp.where(last, a, b)

        def to_west(pair):
            a, b = shift_lanes(pair[0], -1), shift_lanes(pair[1], -1)
            first = iota(a.shape, 1) == 0
            return jnp.where(first, b, a), jnp.where(first, a, b)

        def to_north(pair):
            return shift_rows(pair[0], 1), shift_rows(pair[1], 1)

        def to_south(pair):
            return shift_rows(pair[0], -1), shift_rows(pair[1], -1)

        moves = (to_east, to_west, to_north, to_south)
        def krylov(depth, force, both, cut=None, kept=40):
            moved = [move(depth) for move in moves]
            faces = [[jnp.minimum(depth[t], m[t]) for m in moved] for t in range(2)]
            if cut is not None:
                faces = [[e, w, n, s * cut] for e, w, n, s in faces]
            diag = [2.0 + ((faces[t][0] + faces[t][1]) + (faces[t][2] + faces[t][3])) for t in range(2)]
            inverse = [1.0 / diag[t] for t in range(2)]

            def over_diag(hi, lo, t):
                q, _ = short(hi * inverse[t], 0.0)
                return q, ((hi - diag[t] * q) + lo) * inverse[t]

            vectors = [[short(*over_diag(force[t], 0.0, t)) for t in range(2)]]
            for k in range(4):
                last = vectors[-1]
                high = [move((last[0][0], last[1][0])) for move in moves]
                low = [move((last[0][1], last[1][1])) for move in moves]
                if k == 0 and kept < 40:
                    high, low = ([[x[:kept] for x in pair] for pair in part] for part in (high, low))
                    last = [tuple(x[:kept] for x in pair) for pair in last]
                    faces = [[x[:kept] for x in part] for part in faces]
                    diag, inverse = [x[:kept] for x in diag], [x[:kept] for x in inverse]
                following = []
                for t in range(2 if both or k < 3 else 1):
                    terms = [faces[t][i] * high[i][t] for i in range(4)]
                    fine = [faces[t][i] * low[i][t] for i in range(4)]
                    s0, e0 = two_sum(terms[0], terms[1])
                    s1, e1 = two_sum(terms[2], terms[3])
                    s, e2 = two_sum(s0, s1)
                    rest = ((e0 + e1) + e2) + ((fine[0] + fine[1]) + (fine[2] + fine[3]))
                    q, q_low = over_diag(s, rest, t)
                    s, e = two_sum(last[t][0], -q)
                    following.append(short(s, e + (last[t][1] - q_low)))
                vectors.append(following)
            return diag, vectors

        def counted(pair):
            cells = jnp.where(iota(pair[0].shape, 1) < 128 - HALO, pair[0], pair[1])
            first = jnp.where(sub < HALO, cells[24:32], cells[0:8])
            return jnp.concatenate([first, cells[8:24], jnp.where(sub < southern, cells[0:8], 0.0)], 0)

        southern = jnp.where(lat > 0, 0, HALO)
        cut = jnp.where(iota((40, 128), 0) == 0, has_south, 1.0)
        diag, vectors = krylov(ahead(0), ahead(1), True, cut, 32)
        terms = [tuple(counted((v[0][i], v[1][i])) for i in range(2)) for v in vectors]
        scale = counted(diag)
        weighted = [quick(scale * hi, scale * lo) for hi, lo in terms[:4]]
        terms = [quick(hi, lo) for hi, lo in terms]

        sums = []
        for n in range(8):
            product = dd_mul(weighted[n // 2], terms[n - n // 2])
            tiles = [(product[0][8 * i:8 * i + 8], product[1][8 * i:8 * i + 8]) for i in range(4)]
            sums.append(dd_add(dd_add(tiles[0], tiles[1]), dd_add(tiles[2], tiles[3])))

        def fold(a, b, near_mask, step):
            def one(i):
                x, y = a[i], b[i]
                far = jnp.where(near_mask, pltpu.roll(x, 8 - step, 0), pltpu.roll(y, step, 0))
                return jnp.where(near_mask, x, y), far
            kept, far = zip(*(one(i) for i in range(2)))
            return dd_add(kept, far)

        level = [fold(sums[2 * i], sums[2 * i + 1], sub < 4, 4) for i in range(4)]
        level = [fold(level[2 * i], level[2 * i + 1], sub % 4 < 2, 2) for i in range(2)]
        level = fold(level[0], level[1], sub % 2 < 1, 1)
        parts = [x.T for x in level]
        parts = [tuple(p[8 * i:8 * i + 8] for p in parts) for i in range(16)]
        while len(parts) > 1:
            parts = [dd_add(parts[i], parts[i + 1]) for i in range(0, len(parts), 2)]
        level = parts[0]
        for step in (4, 2, 1):
            level = dd_add(tuple(p[:step] for p in level), tuple(p[step:2 * step] for p in level))
        partial[0:1, 0:8] = level[0]
        partial[1:2, 0:8] = level[1]

        pl.semaphore_wait(ready, len(relay))
        for j, peer in enumerate(line_peer):
            remote(partial, gather_a.at[j], 5, peer).start()
        for d in (N, S):
            rows_copy(d, 1).start()
        surf_copy(NE, (2, 1), surf_b.at[pl.ds(5, 1)], 8).start()
        surf_copy(NW, (2, 1), surf_b.at[pl.ds(4, 1)], 8).start()
        surf_copy(SW, (0, 1), surf_b.at[pl.ds(3, 1)], 8).start()
        surf_copy(W, (0, 3), surf_b.at[pl.ds(0, 3)], 8).start()
        for d in (NE, NW, SE, SW):
            corner_copy(d).start()
        for d in (E, W):
            edge_copy(d).start()

        def total(own, others, number):
            parts = [(own[0:1], own[1:2])] + [(others[j, 0:1], others[j, 1:2]) for j in range(number)]
            while len(parts) > 1:
                parts = [dd_add(parts[i], parts[i + 1]) if i + 1 < len(parts) else parts[i]
                         for i in range(0, len(parts), 2)]
            return parts[0]

        wait_all(recv_sem, 1)
        wait_all(recv_sem, 7)
        south_count, north_count = surf_s[0, 0] * has_south, from_north(0, 0)
        count_own = jnp.concatenate([surf[t, 0] for t in range(3)] + [jnp.where(sub < 4, north_count, south_count)], 0)

        def with_rows(f, block, north, south):
            up = pltpu.roll(north, (8 - 2 * f) % 8, 0) if f else north
            down = pltpu.roll(south, 6 - 2 * f, 0) if f < 3 else south
            return jnp.concatenate([block, jnp.where(sub < 4, up, down)], 0)

        def main(k, slot, rows_in, first, base):
            active = jnp.where(count_own > k.astype(F32), 1.0, 0.0)
            north, south = rows_in[N - 2, k - first], rows_in[S - 2, k - first]
            quads = [with_rows(f, state[f, k], north, south) for f in range(4)]
            for f, value in enumerate(first_pass(active, quads, masked.at[slot], laps.at[k - base], weight.at[k - base])):
                tend[f, k] = value

        def finish(k, base):
            for f in range(4):
                tend[f, k] = tend[f, k] - second_pass(f, laps.at[k - base], weight.at[k - base])

        def unrolled(body, first, last, by):
            def step(i, carry):
                for j in range(by):
                    body(first + i * by + j, j)
                return carry
            lax.fori_loop(0, (last - first) // by, step, 0)

        unrolled(lambda k, slot: main(k, slot, rows_a, 0, 0), 0, quarter, UNROLL)
        wait_all(recv_sem, 10)
        unrolled(lambda k, slot: main(k, slot, rows_c, quarter, 0), quarter, half, UNROLL)
        unrolled(lambda k, slot: finish(k, 0), 0, half, FINISH)

        wait_all(recv_sem, 5)
        hi, lo = total(partial, gather_a, nline - 1)
        mid[0:1] = hi
        mid[1:2] = lo
        for j, peer in enumerate(plane_peer):
            remote(mid, gather_b.at[j], 6, peer).start()

        wait_all(recv_sem, 2)
        unrolled(lambda k, slot: main(k, slot, rows_b, half, half), half, levels, UNROLL)
        unrolled(lambda k, slot: finish(k, half), half, levels, FINISH)
        wait_all(recv_sem, 8)
        depth = around_own(0)
        diag, vectors = krylov(depth, around_own(1), False)
        own_vectors = [quick(v[0][0][:24], v[0][1][:24]) for v in vectors]
        own_diag = diag[0][:24]
        count_side = jnp.concatenate([depth[1][:24], jnp.where(sub < 4, depth[1][24:32], depth[1][32:40])], 0)
        lane32 = iota((32, 128), 1)

        def spread(first, second):
            x = jnp.where(lane32 < 8, jnp.where(lane32 < 4, pltpu.roll(first, 4, 1), pltpu.roll(second, 4, 1)), 0.0)
            for step in (8, 16, 32, 64):
                x = x + pltpu.roll(x, step, 1)
            return x

        counts[0] = spread(count_side, count_own)
        counts[1] = spread(count_own, count_side)

        wait_all(recv_sem, 3)
        wait_all(recv_sem, 4)
        left24, left8 = lane24 % 8 < 4, lane % 8 < 4

        def edge_active(side, g):
            return jnp.where(counts[side] > (lane32 // 8 + g * GROUP).astype(F32), 1.0, 0.0)

        def edge_first(g, side, slot):
            if side == 0:
                north = jnp.where(left8, corners_in[NW - 4, g], rows_b[N - 2, levels - half + g])
                south = jnp.where(left8, corners_in[SW - 4, g], rows_b[S - 2, levels - half + g])
                blocks = [jnp.where(left24, edges_in[W, f, g], edges[f, g]) for f in range(4)]
            else:
                north = jnp.where(left8, rows_b[N - 2, levels - half + g], corners_in[NE - 4, g])
                south = jnp.where(left8, rows_b[S - 2, levels - half + g], corners_in[SE - 4, g])
                blocks = [jnp.where(left24, edges[f, g], edges_in[E, f, g]) for f in range(4)]
            quads = [with_rows(f, blocks[f], north, south) for f in range(4)]
            at = 2 * g + side
            return first_pass(edge_active(side, g), quads, masked.at[slot], laps.at[at], weight.at[at])

        def edge(g):
            west, east = edge_first(g, 0, 0), edge_first(g, 1, 1)
            for f in range(4):
                edge_out[f, g] = jnp.where(left24, east[f], west[f])

        def edge_finish(g):
            for f in range(4):
                west, east = (second_pass(f, laps.at[2 * g + i], weight.at[2 * g + i]) for i in range(2))
                edge_out[f, g] = edge_out[f, g] - jnp.where(left24, east, west)

        unrolled(lambda g, slot: edge(g), 0, groups, 1)
        unrolled(lambda g, slot: edge_finish(g), 0, groups, groups)

        rim = (lane24 < 2) | (lane24 >= 126)

        for k in range(levels):
            g, back = k // GROUP, (252 - 8 * (k % GROUP)) % 128
            for f in range(4):
                pltpu.store(tend.at[f, k], pltpu.roll(edge_out[f, g], back, 1), mask=rim)

        wait_all(recv_sem, 6)
        level = total(mid, gather_b, nplane - 1)

        def scalar(a, n):
            return jnp.broadcast_to(a[0:1, n:n + 1], (8, 128))

        mu = []
        for n in range(8):
            at = 4 * (n % 2) + 2 * (n // 2 % 2) + n // 4
            mu.append((scalar(level[0], at), scalar(level[1], at)))
        x_poly, r_poly = cg_coefficients(mu)
        for t in range(3):
            rows = slice(8 * t, 8 * t + 8)
            basis = [(v[0][rows], v[1][rows]) for v in own_vectors]

            def combined(poly):
                parts = [dd_mul(c, b) for c, b in zip(poly, basis)]
                while len(parts) > 1:
                    parts = [dd_add(parts[i], parts[i + 1]) if i + 1 < len(parts) else parts[i]
                             for i in range(0, len(parts), 2)]
                return parts[0]

            height = combined(x_poly)
            x_ref[rows] = (height[0] + height[1]) * (40.0 / 65536.0)
            rest = combined(r_poly)
            d = own_diag[rows]
            r_ref[rows] = (d * rest[0] + d * rest[1]) * (1.0 / 65536.0)

        for i in (0, 1, 2, 3, 4, 5, 6, 7, 8, 10):
            wait_all(send_sem, i)

        @pl.when(lat > 0)
        def _():
            wait_all(send_sem, 9)


    scratch = [
        pltpu.VMEM((24, 128), F32), pltpu.VMEM((24, 128), jnp.int32), pltpu.VMEM((24, 128), jnp.int32),
        pltpu.VMEM((4, levels, 24, 128), F32),
        pltpu.VMEM((3, 2, 8, 128), F32), pltpu.VMEM((3, 2, 8, 128), F32),
        pltpu.VMEM((1, 2, 8, 128), F32), pltpu.VMEM((6, 2, 8, 128), F32), pltpu.VMEM((4, 2, 8, 128), F32),
        pltpu.VMEM((4, groups, 24, 128), F32), pltpu.VMEM((2, 4, groups, 24, 128), F32),
        pltpu.VMEM((entries, 8, 128), F32), pltpu.VMEM((entries, 8, 128), F32),
        pltpu.VMEM((2, quarter, 8, 128), F32), pltpu.VMEM((2, entries - half, 8, 128), F32),
        pltpu.VMEM((2, half - quarter, 8, 128), F32),
        pltpu.VMEM((4, groups, 8, 128), F32),
        pltpu.VMEM((2, 32, 128), F32), pltpu.VMEM((UNROLL, 4, 48, 128), F32),
        pltpu.VMEM((half, 4, 40, 128), F32), pltpu.VMEM((half, 24, 128), F32),
        pltpu.VMEM((4, groups, 24, 128), F32),
        pltpu.VMEM((2, 128), F32), pltpu.VMEM((nline - 1, 2, 128), F32),
        pltpu.VMEM((2, 128), F32), pltpu.VMEM((nplane - 1, 2, 128), F32),
        pltpu.SemaphoreType.DMA((5,)), pltpu.SemaphoreType.DMA((11,)), pltpu.SemaphoreType.DMA((11,)),
        pltpu.SemaphoreType.REGULAR,
    ]
    return kernel, scratch


def hand_out(x_ref, r_ref, tend_ref, x_out, r_out, tend_out, sem):
    copies = [pltpu.make_async_copy(tend_ref.at[f], tend_out.at[f], sem.at[f]) for f in range(4)]
    copies += [pltpu.make_async_copy(x_ref, x_out, sem.at[4]), pltpu.make_async_copy(r_ref, r_out, sem.at[5])]
    for copy in copies:
        copy.start()
    for copy in copies:
        copy.wait()


def solution(mesh):
    nlon, nlat = mesh.shape["lon"], mesh.shape["lat"]
    nplane = nlon // CORES
    nx = max(n for n in range(1, nplane + 1) if nplane % n == 0 and n * n <= nplane)
    ny = nplane // nx
    finer = Mesh(mesh.devices.reshape(nx, ny, CORES, nlat), ("x", "y", "core", "lat"))

    def per_device(surface_forcing, sea_mask, level_count, state):
        kernel, scratch = make_kernel(nx, ny, nlat, state.shape[1])
        results = pl.pallas_call(
            kernel,
            out_shape=(
                pltpu.VMEM(surface_forcing.shape, F32),
                pltpu.VMEM(surface_forcing.shape, F32),
                pltpu.VMEM(state.shape, F32),
            ),
            in_specs=[pl.BlockSpec(memory_space=pl.ANY)] * 4,
            out_specs=(
                pl.BlockSpec(memory_space=pltpu.VMEM),
                pl.BlockSpec(memory_space=pltpu.VMEM),
                pl.BlockSpec(memory_space=pltpu.VMEM),
            ),
            scratch_shapes=scratch,
            compiler_params=pltpu.CompilerParams(collective_id=0, has_side_effects=True, vmem_limit_bytes=65_030_000),
            name="ocean",
        )(surface_forcing, sea_mask, level_count, state)
        return pl.pallas_call(
            hand_out,
            out_shape=tuple(jax.ShapeDtypeStruct(r.shape, F32) for r in results),
            in_specs=[pl.BlockSpec(memory_space=pltpu.VMEM)] * 3,
            out_specs=[pl.BlockSpec(memory_space=pl.ANY)] * 3,
            scratch_shapes=[pltpu.SemaphoreType.DMA((6,))],
            compiler_params=pltpu.CompilerParams(vmem_limit_bytes=8 * 2**20),
            name="hand_out",
        )(*results)

    flat, deep = P("lat", ("x", "y", "core")), P(None, None, "lat", ("x", "y", "core"))
    return jax.shard_map(
        per_device, mesh=finer, in_specs=(flat, flat, flat, deep), out_specs=(flat, flat, deep), check_vma=False
    )
```
